256 devices in a mesh: dp: 32 (over x, z_lo, core), tensor: 8 (over y, z_hi).
Axes of the slice: x: 4, y: 4, z: 8 (z_hi: 2, z_lo: 4; z = z_hi * 4 + z_lo), core: 2. Of those that a mesh axis runs over, the one named last changes fastest.
Arguments:
- inputs: bfloat16 [32, 1024, 4096], P('dp', 'tensor'), may hold values from -40 to 40
- query_states: bfloat16 [32, 1024, 3072], P('dp', None, 'tensor'), may hold values from -4.5 to 4.5
- key_states: bfloat16 [32, 1024, 1024], P('dp', None, 'tensor'), may hold values from -4.5 to 4.5
- saved_value_states: bfloat16 [32, 1024, 1024], P('dp', None, 'tensor'), may hold values from -4.5 to 4.5
- head_cotangent: bfloat16 [32, 1024, 3072], P('dp', None, 'tensor'), may hold values from -40 to 40
- query_weight: bfloat16 [4096, 3072], P('dp', 'tensor'), may hold values from -0.09375 to 0.09375
- key_matrix: bfloat16 [4096, 1024], P('dp', 'tensor'), may hold values from -0.09375 to 0.09375
- value_matrix: bfloat16 [4096, 1024], P('dp', 'tensor'), may hold values from -0.09375 to 0.09375
- query_momentum: float32 [4096, 3072], P('dp', 'tensor'), may hold values from -6 to 6
- key_prior_momentum: float32 [4096, 1024], P('dp', 'tensor'), may hold values from -6 to 6
- value_prior_momentum: float32 [4096, 1024], P('dp', 'tensor'), may hold values from -6 to 6
Outputs:
- input_gradient: bfloat16 [32, 1024, 4096], P('dp', 'tensor')
- query_velocity: float32 [4096, 3072], P('dp', 'tensor')
- key_velocity: float32 [4096, 1024], P('dp', 'tensor')
- value_velocity: float32 [4096, 1024], P('dp', 'tensor')
The draws below stay inside these ranges and needn't reach their ends.
All inputs are finite; a program needn't handle non-finite values.
Results may differ from the reference program's by a relative error of at most 0.019.
Values may be sent and summed in bfloat16 or wider, within the bound.
A program may use at most 128 MiB of HBM per device.

```python
import math
import jax
import jax.numpy as jnp
from jax import lax

MODEL_FEATURES = 4096
QUERY_HEADS = 24
KEY_VALUE_HEADS = 8
HEAD_SIZE = 128
SEQUENCE_LENGTH = 1024
SEQUENCE_COUNT = 32
N_TENSOR = 8


def column_scales(base_key, width, head_width):
    spread = jnp.exp(jax.random.uniform(base_key, (width,), jnp.float32, math.log(0.3), math.log(3.0)))
    position = (jnp.arange(width, dtype=jnp.int32) // head_width).astype(jnp.float32)
    last_index = max(width // head_width - 1, 1)
    rising = jnp.exp(math.log(3.0) * (position / last_index - 0.5))
    return (spread, rising)


def draw_scaled(base_key, array_shape, head_width):
    key_scale, key_noise = jax.random.split(base_key, 2)
    width = array_shape[-1]
    spread, rising = column_scales(key_scale, width, head_width)
    value_entries = jnp.clip(jax.random.normal(key_noise, array_shape, jnp.float32), -4.0, 4.0) * spread * rising
    return value_entries


def draw_inputs(key, part):
    return draw_scaled(jax.random.fold_in(key, 11), (SEQUENCE_COUNT, SEQUENCE_LENGTH, MODEL_FEATURES), 1).astype(jnp.bfloat16)


def draw_head_cotangent(key, part):
    return draw_scaled(jax.random.fold_in(key, 13), (SEQUENCE_COUNT, SEQUENCE_LENGTH, QUERY_HEADS * HEAD_SIZE), HEAD_SIZE).astype(jnp.bfloat16)


def draw_query_states(key, part):
    base_key = jax.random.fold_in(key, 17)
    array_shape = (SEQUENCE_COUNT, SEQUENCE_LENGTH, QUERY_HEADS, HEAD_SIZE)
    value_entries = jnp.clip(jax.random.normal(base_key, array_shape, jnp.float32), -4.5, 4.5)
    return value_entries.reshape(SEQUENCE_COUNT, SEQUENCE_LENGTH, QUERY_HEADS * HEAD_SIZE).astype(jnp.bfloat16)


def draw_key_states(key, part):
    base_key = jax.random.fold_in(key, 19)
    array_shape = (SEQUENCE_COUNT, SEQUENCE_LENGTH, KEY_VALUE_HEADS, HEAD_SIZE)
    value_entries = jnp.clip(jax.random.normal(base_key, array_shape, jnp.float32), -4.5, 4.5)
    return value_entries.reshape(SEQUENCE_COUNT, SEQUENCE_LENGTH, KEY_VALUE_HEADS * HEAD_SIZE).astype(jnp.bfloat16)


def block_levels(own_key, extent, cuts, low, top_value):
    gain, own = 1.0, jax.random.fold_in(own_key, 6)
    for dim, shards_of in cuts:
        draws = jnp.exp(jax.random.uniform(jax.random.fold_in(own, dim), (shards_of,), jnp.float32, low / len(cuts), top_value / len(cuts)))
        gain = gain * jnp.repeat(draws, extent[dim] // shards_of).reshape([-1 if axis == dim else 1 for axis in range(len(extent))])
    return gain


def scatter_about(rng, extent, deviation, limit, shards=(), kind=jnp.bfloat16):
    values = deviation * jax.random.normal(rng, extent, jnp.float32)
    if shards:
        values = values * block_levels(rng, extent, shards, -0.22, 0.18)
    return jnp.clip(values, -limit, limit).astype(kind)


def setup_inputs(seed: int = 0) -> dict:
    arg_keys = jax.random.split(jax.random.key(seed), 12)
    return {
        "inputs": draw_inputs(jax.random.fold_in(arg_keys[11], 71), 0),
        "query_states": draw_query_states(jax.random.fold_in(arg_keys[11], 71), 0),
        "key_states": draw_key_states(jax.random.fold_in(arg_keys[11], 71), 0),
        "saved_value_states": scatter_about(arg_keys[3], (SEQUENCE_COUNT, SEQUENCE_LENGTH, KEY_VALUE_HEADS * HEAD_SIZE), 1.0, 4.5, ((0, 32), (2, 8))),
        "head_cotangent": draw_head_cotangent(jax.random.fold_in(arg_keys[11], 71), 0),
        "query_weight": scatter_about(arg_keys[5], (MODEL_FEATURES, QUERY_HEADS * HEAD_SIZE), MODEL_FEATURES ** -0.5, 0.09375, ((0, 32), (1, 8))),
        "key_matrix": scatter_about(arg_keys[6], (MODEL_FEATURES, KEY_VALUE_HEADS * HEAD_SIZE), MODEL_FEATURES ** -0.5, 0.09375, ((0, 32), (1, 8))),
        "value_matrix": scatter_about(arg_keys[7], (MODEL_FEATURES, KEY_VALUE_HEADS * HEAD_SIZE), MODEL_FEATURES ** -0.5, 0.09375, ((0, 32), (1, 8))),
        "query_momentum": scatter_about(arg_keys[8], (MODEL_FEATURES, QUERY_HEADS * HEAD_SIZE), 1.0, 6.0, ((0, 32), (1, 8)), jnp.float32),
        "key_prior_momentum": scatter_about(arg_keys[9], (MODEL_FEATURES, KEY_VALUE_HEADS * HEAD_SIZE), 1.0, 6.0, ((0, 32), (1, 8)), jnp.float32),
        "value_prior_momentum": scatter_about(arg_keys[10], (MODEL_FEATURES, KEY_VALUE_HEADS * HEAD_SIZE), 1.0, 6.0, ((0, 32), (1, 8)), jnp.float32),
    }


def rounded(value_entries):
    return lax.optimization_barrier(value_entries.astype(jnp.bfloat16)).astype(jnp.float32)

def sequence_backward(sequence_queries, sequence_keys, sequence_values, sequence_cotangent):
    token_length = sequence_queries.shape[0]
    group_width = QUERY_HEADS // KEY_VALUE_HEADS
    scaling = 1.0 / math.sqrt(HEAD_SIZE)
    query_quad = sequence_queries.astype(jnp.float32).reshape(token_length, KEY_VALUE_HEADS, group_width, HEAD_SIZE)
    cotangent_quad = sequence_cotangent.astype(jnp.float32).reshape(token_length, KEY_VALUE_HEADS, group_width, HEAD_SIZE)
    key_triple = sequence_keys.astype(jnp.float32).reshape(token_length, KEY_VALUE_HEADS, HEAD_SIZE)
    value_triple = sequence_values.astype(jnp.float32).reshape(token_length, KEY_VALUE_HEADS, HEAD_SIZE)
    scores = jnp.einsum('ihgd,jhd->hgij', query_quad, key_triple) * scaling
    position = jnp.arange(token_length, dtype=jnp.int32)
    causal = position[:, None] >= position[None, :]
    scores = jnp.where(causal, scores, -jnp.inf)
    maximum = lax.optimization_barrier(jnp.max(scores, axis=-1, keepdims=True))
    exponent = jnp.exp(scores - maximum)
    softmax_rows = exponent / lax.optimization_barrier(jnp.sum(exponent, axis=-1, keepdims=True))
    softmax_reduced = rounded(softmax_rows)
    grad_softmax = jnp.einsum('ihgd,jhd->hgij', cotangent_quad, value_triple)
    row_delta = lax.optimization_barrier(jnp.sum(softmax_rows * grad_softmax, axis=-1, keepdims=True))
    score_gradient = rounded(softmax_rows * (grad_softmax - row_delta) * scaling)
    grad_query = jnp.einsum('hgij,jhd->ihgd', score_gradient, key_triple).astype(jnp.bfloat16).reshape(token_length, QUERY_HEADS * HEAD_SIZE)
    key_gradient = jnp.einsum('xfwo,wxfp->oxp', score_gradient, query_quad).astype(jnp.bfloat16).reshape(token_length, KEY_VALUE_HEADS * HEAD_SIZE)
    value_gradient = jnp.einsum('xfwo,wxfp->oxp', softmax_reduced, cotangent_quad).astype(jnp.bfloat16).reshape(token_length, KEY_VALUE_HEADS * HEAD_SIZE)
    return (grad_query, key_gradient, value_gradient)

def reference(inputs, query_states, key_states, saved_value_states, head_cotangent, query_weight, key_matrix, value_matrix, query_momentum, key_prior_momentum, value_prior_momentum):
    query_share = QUERY_HEADS * HEAD_SIZE // N_TENSOR
    paired_portion = KEY_VALUE_HEADS * HEAD_SIZE // N_TENSOR

    def one_sequence(running, sequence_slices):
        input_seq, sequence_queries, sequence_keys, sequence_values, sequence_cotangent = sequence_slices
        grad_query, key_gradient, value_gradient = sequence_backward(sequence_queries, sequence_keys, sequence_values, sequence_cotangent)
        summed = jnp.zeros((input_seq.shape[0], MODEL_FEATURES), jnp.float32)
        for block_index in range(N_TENSOR):
            query_span = slice(block_index * query_share, (block_index + 1) * query_share)
            pair_span = slice(block_index * paired_portion, (block_index + 1) * paired_portion)
            partial_value = jnp.dot(grad_query[:, query_span], query_weight[:, query_span].T, preferred_element_type=jnp.float32)
            partial_value = partial_value + jnp.dot(key_gradient[:, pair_span], key_matrix[:, pair_span].T, preferred_element_type=jnp.float32)
            partial_value = partial_value + jnp.dot(value_gradient[:, pair_span], value_matrix[:, pair_span].T, preferred_element_type=jnp.float32)
            summed = summed + rounded(partial_value)
        running_query, running_key, running_value = running
        input_trans = input_seq.T
        running_query = running_query + rounded(jnp.dot(input_trans, grad_query, preferred_element_type=jnp.float32))
        running_key = running_key + rounded(jnp.dot(input_trans, key_gradient, preferred_element_type=jnp.float32))
        running_value = running_value + rounded(jnp.dot(input_trans, value_gradient, preferred_element_type=jnp.float32))
        return ((running_query, running_key, running_value), summed.astype(jnp.bfloat16))
    initial_state = (jnp.zeros((MODEL_FEATURES, QUERY_HEADS * HEAD_SIZE), jnp.float32), jnp.zeros((MODEL_FEATURES, KEY_VALUE_HEADS * HEAD_SIZE), jnp.float32), jnp.zeros((MODEL_FEATURES, KEY_VALUE_HEADS * HEAD_SIZE), jnp.float32))
    sums, input_gradient = lax.scan(one_sequence, initial_state, (inputs, query_states, key_states, saved_value_states, head_cotangent))
    grad_w_query, grad_w_key, grad_w_value = sums
    squared_total = jnp.sum(grad_w_query * grad_w_query) + jnp.sum(grad_w_key * grad_w_key) + jnp.sum(grad_w_value * grad_w_value)
    root_mean_square = jnp.sqrt(squared_total / (MODEL_FEATURES * (QUERY_HEADS + 2 * KEY_VALUE_HEADS) * HEAD_SIZE))
    factor = 1.0 / jnp.maximum(root_mean_square, 1.0)
    query_velocity = 0.9 * query_momentum + factor * grad_w_query
    key_velocity = 0.9 * key_prior_momentum + factor * grad_w_key
    value_velocity = 0.9 * value_prior_momentum + factor * grad_w_value
    return (input_gradient, query_velocity, key_velocity, value_velocity)
```

```python
import functools
import math

import jax
import jax.numpy as jnp
from jax import lax
from jax.experimental import pallas as pl
from jax.experimental.pallas import tpu as pltpu
from jax.sharding import Mesh
from jax.sharding import PartitionSpec as P

MODEL_FEATURES = 4096
QUERY_HEADS = 24
KEY_VALUE_HEADS = 8
HEAD = 128
DP = ("dp_0", "dp_1", "dp_2")
TENSOR = ("tensor_0", "tensor_1")
AXES = DP + TENSOR
MESH = pl.DeviceIdType.MESH
BF = jnp.bfloat16
F32 = jnp.float32

COLS = 640
ALL = 4 * COLS
QB = 256


def dot(a, b, ca, cb):
    return lax.dot_general(a, b, (((ca,), (cb,)), ((), ())), preferred_element_type=F32)


def lanes(start, size):
    return pl.ds(pl.multiple_of(start, 128), size)


def kernel(
    in_ref, q_ref, k_ref, v_ref, do_ref, wq_ref, wk_ref, wv_ref, mq_ref, mk_ref, mv_ref,
    gx_ref, vq_ref, vk_ref, vv_ref,
    xq, xt, g, w, s_buf, dp_buf, p_buf, ds_buf, dk_acc, dv_acc,
    dw_cs, dw_cr, dw_xs, dw_xr, dw_acc, dw_zs, dw_zr, dw_fin, dw_sw, dw_gr,
    dx_s, dx_r, dx_o, dx_f, sq1, sq2,
    ws_s, ws_r, wz_s, wz_r, wx_s, wx_r, wc_s, wc_r,
    xy_s, xy_r, xz_s, xz_r, go_s, go_r, gf_s, gf_r,
    dc_s, dc_r, dxx_s, dxx_r, dz_s, dz_r, dsw_s, dsw_r,
    ez_s, ez_r, ey_s, ey_r, s1_s, s1_r, s2_s, s2_r,
):
    x, zl, c, y, zh = (lax.axis_index(a) for a in AXES)
    scaling = 1.0 / math.sqrt(HEAD)
    other_c, other_zh = 1 - c, 1 - zh

    def at(dx=0, dl=0, dy=0):
        return (lax.rem(x + dx, 4), lax.rem(zl + dl, 4), c, lax.rem(y + dy, 4), zh)

    swap_dev = (y, zl, c, x, zh)
    core_dev = (x, zl, other_c, y, zh)
    zh_dev = (x, zl, c, y, other_zh)

    def line(dz, dc):
        z = lax.rem(zh * 4 + zl + dz, 8)
        return (x, lax.rem(z, 4), lax.rem(c + dc, 2), y, z // 4)

    plane = [(dx, dy) for dx in range(4) for dy in range(4) if dx or dy]
    column = [(dz, dc) for dz in range(8) for dc in range(2) if dz or dc]

    def send(src, dst, ss, rs, dev):
        return pltpu.make_async_remote_copy(
            src_ref=src, dst_ref=dst, send_sem=ss, recv_sem=rs, device_id=dev, device_id_type=MESH
        )

    barrier = pltpu.get_barrier_semaphore()
    for dx, dy in plane:
        pl.semaphore_signal(barrier, inc=1, device_id=at(dx=dx, dy=dy), device_id_type=MESH)
    for dz, dc in column:
        pl.semaphore_signal(barrier, inc=1, device_id=line(dz, dc), device_id_type=MESH)
    pl.semaphore_wait(barrier, 30)

    w_rows = pl.ds(zl * 128, 128)
    w_parts = ((wq_ref, 0, 384), (wk_ref, 384, 128), (wv_ref, 512, 128))

    def w_swap(n):
        ref, off, size = w_parts[n]
        dst = w.at[c, w_rows, lanes(y * COLS + off, size)]
        return send(ref, dst, ws_s.at[n], ws_r.at[n], swap_dev)

    def w_near(n):
        own = w.at[c, w_rows, lanes(x * COLS, COLS)]
        return send(own, own, wz_s.at[n], wz_r.at[n], at(dl=n + 1))

    def w_far(n):
        own = w.at[c, :, lanes(x * COLS, COLS)]
        return send(own, own, wx_s.at[n], wx_r.at[n], at(dx=n + 1))

    def w_core():
        return send(w.at[c], w.at[c], wc_s, wc_r, core_dev)

    @pl.when(x != y)
    def _():
        for n in range(3):
            w_swap(n).start()

    @pl.when(x == y)
    def _():
        for ref, off, size in w_parts:
            w[c, w_rows, lanes(x * COLS + off, size)] = ref[...]

    def x_rows(dy):
        return pl.ds((2 * lax.rem(y + 4 - dy, 4) + zh) * 128, 128)

    def x_y(n):
        to = lax.rem(y + n + 1, 4)
        return send(
            in_ref.at[0, :, lanes(to * 1024, 1024)], xq.at[x_rows(0)],
            xy_s.at[n], xy_r.at[n], at(dy=n + 1),
        )

    def x_z(n):
        rows = xq.at[x_rows(n)]
        return send(rows, rows, xz_s.at[n], xz_r.at[n], zh_dev)

    own_x = in_ref.at[0, :, lanes(y * 1024, 1024)]
    send(own_x, xq.at[x_rows(0)], xz_s.at[0], xz_r.at[0], zh_dev).start()
    for n in range(3):
        x_y(n).start()
    xq[x_rows(0), :] = own_x[...]

    def g_own(p, d):
        piece = g.at[:, :, :, lanes(y * COLS + p * 128, 128)]
        return send(piece, piece, go_s.at[d, p], go_r.at[d, p], at(dy=1 if d == 0 else 3))

    def g_forward(p, d):
        of = lax.rem(y + (3 if d == 0 else 1), 4)
        half = g.at[2 * d : 2 * d + 2, :, :, lanes(of * COLS + p * 128, 128)]
        return send(half, half, gf_s.at[d, p], gf_r.at[d, p], at(dy=1 if d == 0 else 3))

    dk_acc[...] = jnp.zeros_like(dk_acc)
    dv_acc[...] = jnp.zeros_like(dv_acc)
    causal = lax.broadcasted_iota(jnp.int32, (QB, QB), 0) <= lax.broadcasted_iota(
        jnp.int32, (QB, QB), 1
    )

    def head(h, _):
        cols = lanes(h * HEAD, HEAD)
        for i in range(4):
            rows = pl.ds(i * QB, QB)
            qi, doi = q_ref[0, rows, cols], do_ref[0, rows, cols]
            width = (i + 1) * QB
            top = None
            for j in range(i + 1):
                js = pl.ds(j * QB, QB)
                s = dot(k_ref[0, js, :], qi, 1, 1) * scaling
                if j == i:
                    s = jnp.where(causal, s, -jnp.inf)
                s_buf[js, :] = s
                m = jnp.max(s, axis=0, keepdims=True)
                top = m if top is None else jnp.maximum(top, m)
            total = jnp.zeros((1, QB), F32)
            delta = jnp.zeros((1, QB), F32)
            for j in range(i + 1):
                js = pl.ds(j * QB, QB)
                e = jnp.exp(s_buf[js, :] - top)
                dp = dot(v_ref[0, js, :], doi, 1, 1)
                s_buf[js, :] = e
                dp_buf[js, :] = dp
                total = total + jnp.sum(e, axis=0, keepdims=True)
                delta = delta + jnp.sum(e * dp, axis=0, keepdims=True)
            inverse = 1.0 / total
            delta = delta * inverse
            for j in range(i + 1):
                js = pl.ds(j * QB, QB)
                p = s_buf[js, :] * inverse
                p_buf[js, :] = p.astype(BF)
                ds_buf[js, :] = (p * (dp_buf[js, :] - delta) * scaling).astype(BF)
            dv_acc[:width, :] += dot(p_buf[:width, :], doi, 1, 0)
            dk_acc[:width, :] += dot(ds_buf[:width, :], qi, 1, 0)
            dq = dot(ds_buf[:width, :], k_ref[0, :width, :], 0, 0).astype(BF)
            g[i, :, :, lanes(y * COLS + h * HEAD, HEAD)] = dq.reshape(2, 128, HEAD)
        g_own(h, 0).start()
        g_own(h, 1).start()

        @pl.when(h == 0)
        def _():
            @pl.when(x != y)
            def _():
                for n in range(3):
                    w_swap(n).wait()

            for n in range(3):
                w_near(n).start()

        return 0

    lax.fori_loop(0, 3, head, 0)
    for p, acc in ((3, dk_acc), (4, dv_acc)):
        g[:, :, :, lanes(y * COLS + p * 128, 128)] = acc[...].astype(BF).reshape(4, 2, 128, 128)
        g_own(p, 0).start()
        g_own(p, 1).start()
    for n in range(3):
        x_y(n).wait_recv()
        x_z(n + 1).start()
    for n in range(3):
        w_near(n).wait()
    for n in range(3):
        w_far(n).start()

    def turn(t, _):
        rows = pl.ds(pl.multiple_of(t * 128, 128), 128)
        for b in range(8):
            block = xq[rows, b * 128 : b * 128 + 128]
            xt[b % 2, (b // 2) * 128 : (b // 2) * 128 + 128, lanes(t * 128, 128)] = block.T
        return 0

    for p in range(5):
        for d in range(2):
            g_own(p, d).wait_recv()
            g_forward(p, d).start()
    lax.fori_loop(0, 4, lambda b, _: turn(2 * b + zh, 0), 0)
    for n in range(4):
        x_z(n).wait_recv()
    lax.fori_loop(0, 4, lambda b, _: turn(2 * b + other_zh, 0), 0)
    for n in range(3):
        w_far(n).wait()
    w_core().start()
    for p in range(5):
        for d in range(2):
            g_forward(p, d).wait_recv()

    def d_core(k):
        return send(dw_cs.at[k], dw_cr.at[k], dc_s.at[k], dc_r.at[k], core_dev)

    def d_x(n):
        return send(dw_xs.at[n], dw_xr.at[n], dxx_s.at[n], dxx_r.at[n], at(dx=n + 1))

    def d_z(n):
        return send(dw_zs.at[n], dw_zr.at[n], dz_s.at[n], dz_r.at[n], at(dl=n + 1))

    def d_swap():
        return send(dw_sw, dw_gr, dsw_s, dsw_r, swap_dev)

    def product(half, n):
        k = lax.rem(x + 1 + n, 4)
        rhs = g[:, :, :, lanes(k * COLS, COLS)].reshape(1024, COLS)
        return dot(xt[half], rhs, 1, 0)

    def for_core(n, _):
        dw_cs[n] = product(other_c, n).astype(BF)
        d_core(n).start()
        return 0

    def for_x(n, _):
        part = product(c, n)
        d_core(n).wait_recv()
        part = part + dw_cr[n].astype(F32)

        @pl.when(n < 3)
        def _():
            dw_xs[n] = part.astype(BF)
            d_x(n).start()

        @pl.when(n == 3)
        def _():
            dw_acc[...] = part

        return 0

    lax.fori_loop(0, 4, for_core, 0)
    lax.fori_loop(0, 4, for_x, 0)

    def e_z(n):
        to = lax.rem(y + 1 + n, 4)
        return send(dx_s.at[to], dx_r.at[to], ez_s.at[n], ez_r.at[n], zh_dev)

    def e_y(n):
        dst = gx_ref.at[0, :, lanes(y * 1024, 1024)]
        return send(dx_f.at[n], dst, ey_s.at[n], ey_r.at[n], at(dy=n + 1))

    def back(tokens, half):
        return dot(g[:, tokens].reshape(512, ALL), w[half], 1, 1)

    w_core().wait()
    for half in range(2):
        r = back(other_zh, half).astype(BF).reshape(4, 128, 512)
        for b in range(4):
            dx_s[:, :, b * 256 + half * 128 : b * 256 + half * 128 + 128] = r[:, :, b * 128 : b * 128 + 128]
    for n in range(3):
        e_z(n).start()
    for half in range(2):
        r = back(zh, half).reshape(4, 128, 512)
        for b in range(4):
            dx_o[:, :, b * 256 + half * 128 : b * 256 + half * 128 + 128] = r[:, :, b * 128 : b * 128 + 128]

    def finish(n):
        e_z(n).wait_recv()
        to = lax.rem(y + 1 + n, 4)
        done = (dx_o[to] + dx_r[to].astype(F32)).astype(BF)
        if n < 3:
            dx_f[n] = done
            e_y(n).start()
        else:
            gx_ref[0, :, lanes(y * 1024, 1024)] = done

    finish(0)
    finish(1)
    for n in range(3):
        d_x(n).wait_recv()

    def summed(rows):
        r = dw_acc[rows, :]
        for n in range(3):
            r = r + dw_xr[n, rows, :].astype(F32)
        return r

    for n in range(3):
        dw_zs[n] = summed(pl.ds(lax.rem(zl + n + 1, 4) * 128, 128)).astype(BF)
        d_z(n).start()
    e_z(3).start()
    dw_fin[...] = summed(pl.ds(zl * 128, 128))
    finish(2)
    for n in range(3):
        d_z(n).wait_recv()
    grad = dw_fin[...]
    for n in range(3):
        grad = grad + dw_zr[n].astype(F32)
    dw_sw[...] = grad.astype(BF)

    @pl.when(x != y)
    def _():
        d_swap().start()

    @pl.when(x == y)
    def _():
        dw_gr[...] = dw_sw[...]

    def s_plane(n):
        return send(sq1.at[0], sq1.at[n + 1], s1_s.at[n], s1_r.at[n], at(dx=plane[n][0], dy=plane[n][1]))

    def s_column(n):
        return send(sq2.at[0], sq2.at[n + 1], s2_s.at[n], s2_r.at[n], line(*column[n]))

    squares = jnp.sum((grad * grad).reshape(16, 8, COLS), axis=0)
    sq1[0] = sum(squares[:, b * 128 : b * 128 + 128] for b in range(5))
    for n in range(15):
        s_plane(n).start()
    for n in range(15):
        s_plane(n).wait_recv()
    sq2[0] = jnp.sum(sq1[...], axis=0)
    for n in range(15):
        s_column(n).start()
    for n in range(15):
        s_column(n).wait_recv()
    squared_total = jnp.sum(jnp.sum(sq2[...], axis=0), keepdims=True)
    entries = MODEL_FEATURES * (QUERY_HEADS + 2 * KEY_VALUE_HEADS) * HEAD
    factor = 1.0 / jnp.maximum(jnp.sqrt(squared_total / entries), 1.0)

    @pl.when(x != y)
    def _():
        d_swap().wait()

    vq_ref[...] = 0.9 * mq_ref[...] + factor * dw_gr[:, :384].astype(F32)
    vk_ref[...] = 0.9 * mk_ref[...] + factor * dw_gr[:, 384:512].astype(F32)
    vv_ref[...] = 0.9 * mv_ref[...] + factor * dw_gr[:, 512:].astype(F32)
    finish(3)

    for n in range(3):
        e_y(n).wait()
        x_y(n).wait_send()
        d_x(n).wait_send()
        d_z(n).wait_send()
    for n in range(4):
        x_z(n).wait_send()
        d_core(n).wait_send()
        e_z(n).wait_send()
    for p in range(5):
        for d in range(2):
            g_own(p, d).wait_send()
            g_forward(p, d).wait_send()
    for n in range(15):
        s_plane(n).wait_send()
        s_column(n).wait_send()


def local(*args):
    vm = pltpu.VMEM
    scratch = [
        vm((1024, 1024), BF), vm((2, 512, 1024), BF), vm((4, 2, 128, ALL), BF), vm((2, 512, ALL), BF),
        vm((1024, QB), F32), vm((1024, QB), F32), vm((1024, QB), BF), vm((1024, QB), BF),
        vm((1024, HEAD), F32), vm((1024, HEAD), F32),
        vm((4, 512, COLS), BF), vm((4, 512, COLS), BF), vm((3, 512, COLS), BF), vm((3, 512, COLS), BF),
        vm((512, COLS), F32), vm((3, 128, COLS), BF), vm((3, 128, COLS), BF), vm((128, COLS), F32),
        vm((128, COLS), BF), vm((128, COLS), BF),
        vm((4, 128, 1024), BF), vm((4, 128, 1024), BF), vm((4, 128, 1024), F32), vm((3, 128, 1024), BF),
        vm((16, 8, 128), F32), vm((16, 8, 128), F32),
    ]
    shapes = [(3,), (3,), (3,), (), (3,), (4,), (2, 5), (2, 5), (4,), (3,), (3,), (), (4,), (3,), (15,), (15,)]
    for shape in shapes:
        scratch += [pltpu.SemaphoreType.DMA(shape)] * 2
    whole = pl.BlockSpec(memory_space=pltpu.VMEM)
    return pl.pallas_call(
        kernel,
        out_shape=(
            jax.ShapeDtypeStruct((1, 128, MODEL_FEATURES), BF),
            jax.ShapeDtypeStruct((128, 384), F32),
            jax.ShapeDtypeStruct((128, 128), F32),
            jax.ShapeDtypeStruct((128, 128), F32),
        ),
        in_specs=[whole] * 11,
        out_specs=(whole,) * 4,
        scratch_shapes=scratch,
        compiler_params=pltpu.CompilerParams(
            collective_id=0, has_side_effects=True, vmem_limit_bytes=62 * 1024 * 1024
        ),
        name="block",
    )(*args)


def solution(mesh):
    torus = Mesh(mesh.devices.reshape(4, 4, 2, 4, 2), AXES)
    in_specs = (
        P(DP, TENSOR, None),
        P(DP, None, TENSOR),
        P(DP, None, TENSOR),
        P(DP, None, TENSOR),
        P(DP, None, TENSOR),
        P(DP, TENSOR),
        P(DP, TENSOR),
        P(DP, TENSOR),
        P(DP, TENSOR),
        P(DP, TENSOR),
        P(DP, TENSOR),
    )
    out_specs = (P(DP, TENSOR, None), P(DP, TENSOR), P(DP, TENSOR), P(DP, TENSOR))
    return jax.shard_map(local, mesh=torus, in_specs=in_specs, out_specs=out_specs, check_vma=False)
```

```python
import functools
import math

import jax
import jax.numpy as jnp
from jax import lax
from jax.experimental import pallas as pl
from jax.experimental.pallas import tpu as pltpu
from jax.sharding import Mesh
from jax.sharding import PartitionSpec as P

MODEL_FEATURES = 4096
QUERY_HEADS = 24
KEY_VALUE_HEADS = 8
HEAD = 128
DP = ("dp_0", "dp_1", "dp_2")
TENSOR = ("tensor_0", "tensor_1")
AXES = DP + TENSOR
MESH = pl.DeviceIdType.MESH
BF = jnp.bfloat16
F32 = jnp.float32

COLS = 640
ALL = 4 * COLS
QB = 256


def dot(a, b, ca, cb):
    return lax.dot_general(a, b, (((ca,), (cb,)), ((), ())), preferred_element_type=F32)


def lanes(start, size):
    return pl.ds(pl.multiple_of(start, 128), size)


def kernel(
    in_ref, q_hbm, k_hbm, v_hbm, do_hbm, wq_ref, wk_ref, wv_ref, mq_hbm, mk_hbm, mv_hbm,
    gx_ref, vq_ref, vk_ref, vv_ref,
    q_ref, k_ref, v_ref, do_ref, mq_ref, mk_ref, mv_ref, l_sem, lw_sem, lx_sem,
    xq, xt, g, w, s_buf, dp_buf, p_buf, ds_buf, dk_acc, dv_acc,
    dw_cs, dw_cr, dw_xs, dw_xr, dw_acc, dw_zs, dw_zr, dw_fin, dw_sw, dw_gr,
    dx_s, dx_r, dx_o, dx_f, sq1, sq2,
    ws_s, ws_r, wz_s, wz_r, wx_s, wx_r, wc_s, wc_r,
    xy_s, xy_r, xz_s, xz_r, go_s, go_r, gf_s, gf_r,
    dc_s, dc_r, dxx_s, dxx_r, dz_s, dz_r, dsw_s, dsw_r,
    ez_s, ez_r, ey_s, ey_r, s1_s, s1_r, s2_s, s2_r,
):
    x, zl, c, y, zh = (lax.axis_index(a) for a in AXES)
    scaling = 1.0 / math.sqrt(HEAD)
    other_c, other_zh = 1 - c, 1 - zh

    def at(dx=0, dl=0, dy=0):
        return (lax.rem(x + dx, 4), lax.rem(zl + dl, 4), c, lax.rem(y + dy, 4), zh)

    swap_dev = (y, zl, c, x, zh)
    core_dev = (x, zl, other_c, y, zh)
    zh_dev = (x, zl, c, y, other_zh)

    def line(dz, dc):
        z = lax.rem(zh * 4 + zl + dz, 8)
        return (x, lax.rem(z, 4), lax.rem(c + dc, 2), y, z // 4)

    plane = [(dx, dy) for dx in range(4) for dy in range(4) if dx or dy]
    column = [(dz, dc) for dz in range(8) for dc in range(2) if dz or dc]

    def send(src, dst, ss, rs, dev):
        return pltpu.make_async_remote_copy(
            src_ref=src, dst_ref=dst, send_sem=ss, recv_sem=rs, device_id=dev, device_id_type=MESH
        )

    barrier = pltpu.get_barrier_semaphore()
    for dx, dy in plane:
        pl.semaphore_signal(barrier, inc=1, device_id=at(dx=dx, dy=dy), device_id_type=MESH)
    for dz, dc in column:
        pl.semaphore_signal(barrier, inc=1, device_id=line(dz, dc), device_id_type=MESH)
    loads = [
        pltpu.make_async_copy(src, dst, l_sem.at[n])
        for n, (src, dst) in enumerate(
            (
                (q_hbm, q_ref), (k_hbm, k_ref), (v_hbm, v_ref), (do_hbm, do_ref),
                (mq_hbm, mq_ref), (mk_hbm, mk_ref), (mv_hbm, mv_ref),
            )
        )
    ]
    for load in loads:
        load.start()
    pl.semaphore_wait(barrier, 30)

    w_rows = pl.ds(zl * 128, 128)
    w_parts = ((wq_ref, 0, 384), (wk_ref, 384, 128), (wv_ref, 512, 128))

    def w_swap(n):
        ref, off, size = w_parts[n]
        dst = w.at[c, w_rows, lanes(y * COLS + off, size)]
        return send(ref, dst, ws_s.at[n], ws_r.at[n], swap_dev)

    def w_here(n):
        ref, off, size = w_parts[n]
        return pltpu.make_async_copy(ref, w.at[c, w_rows, lanes(x * COLS + off, size)], lw_sem.at[n])

    def w_near(n):
        own = w.at[c, w_rows, lanes(x * COLS, COLS)]
        return send(own, own, wz_s.at[n], wz_r.at[n], at(dl=n + 1))

    def w_far(m, n):
        block = w.at[c, pl.ds(lax.rem(zl + 4 - m, 4) * 128, 128), lanes(x * COLS, COLS)]
        return send(block, block, wx_s.at[m, n], wx_r.at[m, n], at(dx=n + 1))

    def w_core(n):
        part = w.at[c, :, lanes(lax.rem(x + 4 - n, 4) * COLS, COLS)]
        return send(part, part, wc_s.at[n], wc_r.at[n], core_dev)

    @pl.when(x != y)
    def _():
        for n in range(3):
            w_swap(n).start()

    @pl.when(x == y)
    def _():
        for n in range(3):
            w_here(n).start()

    def x_rows(dy):
        return pl.ds((2 * lax.rem(y + 4 - dy, 4) + zh) * 128, 128)

    def x_y(n):
        to = lax.rem(y + n + 1, 4)
        return send(
            in_ref.at[0, :, lanes(to * 1024, 1024)], xq.at[x_rows(0)],
            xy_s.at[n], xy_r.at[n], at(dy=n + 1),
        )

    def x_z(n):
        rows = xq.at[x_rows(n)]
        return send(rows, rows, xz_s.at[n], xz_r.at[n], zh_dev)

    own_x = in_ref.at[0, :, lanes(y * 1024, 1024)]
    send(own_x, xq.at[x_rows(0)], xz_s.at[0], xz_r.at[0], zh_dev).start()
    for n in range(3):
        x_y(n).start()
    x_here = pltpu.make_async_copy(own_x, xq.at[x_rows(0)], lx_sem)
    x_here.start()
    for load in loads[:4]:
        load.wait()

    def g_own(p, d):
        piece = g.at[:, :, :, lanes(y * COLS + p * 128, 128)]
        return send(piece, piece, go_s.at[d, p], go_r.at[d, p], at(dy=1 if d == 0 else 3))

    def g_forward(p, d):
        of = lax.rem(y + (3 if d == 0 else 1), 4)
        half = g.at[2 * d : 2 * d + 2, :, :, lanes(of * COLS + p * 128, 128)]
        return send(half, half, gf_s.at[d, p], gf_r.at[d, p], at(dy=1 if d == 0 else 3))

    dk_acc[...] = jnp.zeros_like(dk_acc)
    dv_acc[...] = jnp.zeros_like(dv_acc)
    causal = lax.broadcasted_iota(jnp.int32, (QB, QB), 0) <= lax.broadcasted_iota(
        jnp.int32, (QB, QB), 1
    )

    def head(h, _):
        cols = lanes(h * HEAD, HEAD)
        for i in range(4):
            rows = pl.ds(i * QB, QB)
            qi, doi = q_ref[0, rows, cols], do_ref[0, rows, cols]
            width = (i + 1) * QB
            top = None
            for j in range(i + 1):
                js = pl.ds(j * QB, QB)
                s = dot(k_ref[0, js, :], qi, 1, 1) * scaling
                if j == i:
                    s = jnp.where(causal, s, -jnp.inf)
                s_buf[js, :] = s
                m = jnp.max(s, axis=0, keepdims=True)
                top = m if top is None else jnp.maximum(top, m)
            total = jnp.zeros((1, QB), F32)
            delta = jnp.zeros((1, QB), F32)
            for j in range(i + 1):
                js = pl.ds(j * QB, QB)
                e = jnp.exp(s_buf[js, :] - top)
                dp = dot(v_ref[0, js, :], doi, 1, 1)
                s_buf[js, :] = e
                dp_buf[js, :] = dp
                total = total + jnp.sum(e, axis=0, keepdims=True)
                delta = delta + jnp.sum(e * dp, axis=0, keepdims=True)
            inverse = 1.0 / total
            delta = delta * inverse
            for j in range(i + 1):
                js = pl.ds(j * QB, QB)
                p = s_buf[js, :] * inverse
                p_buf[js, :] = p.astype(BF)
                ds_buf[js, :] = (p * (dp_buf[js, :] - delta) * scaling).astype(BF)
            dv_acc[:width, :] += dot(p_buf[:width, :], doi, 1, 0)
            dk_acc[:width, :] += dot(ds_buf[:width, :], qi, 1, 0)
            dq = dot(ds_buf[:width, :], k_ref[0, :width, :], 0, 0).astype(BF)
            g[i, :, :, lanes(y * COLS + h * HEAD, HEAD)] = dq.reshape(2, 128, HEAD)
        @pl.when(h == 0)
        def _():
            @pl.when(x != y)
            def _():
                for n in range(3):
                    w_swap(n).wait()

            @pl.when(x == y)
            def _():
                for n in range(3):
                    w_here(n).wait()

            for n in range(3):
                w_near(n).start()
            for n in range(3):
                w_far(0, n).start()

        g_own(h, 0).start()
        g_own(h, 1).start()
        return 0

    lax.fori_loop(0, 3, head, 0)
    for p, acc in ((3, dk_acc), (4, dv_acc)):
        g[:, :, :, lanes(y * COLS + p * 128, 128)] = acc[...].astype(BF).reshape(4, 2, 128, 128)
        g_own(p, 0).start()
        g_own(p, 1).start()
    def turn(t, _):
        rows = pl.ds(pl.multiple_of(t * 128, 128), 128)
        for b in range(8):
            block = xq[rows, b * 128 : b * 128 + 128]
            xt[b % 2, (b // 2) * 128 : (b // 2) * 128 + 128, lanes(t * 128, 128)] = block.T
        return 0

    for n in range(3):
        x_y(n).wait_recv()
    def forward(p):
        for d in range(2):
            g_own(p, d).wait_recv()
            g_forward(p, d).start()

    def spread(n):
        w_near(n).wait_recv()
        for to in range(3):
            w_far(n + 1, to).start()

    forward(0)
    for n in range(3):
        x_z(n + 1).start()
    forward(1)
    spread(0)
    forward(2)
    spread(1)
    forward(3)
    spread(2)
    forward(4)
    w_core(0).start()
    x_here.wait()
    lax.fori_loop(0, 4, lambda b, _: turn(2 * b + zh, 0), 0)
    for n in range(3):
        for m in range(4):
            w_far(m, n).wait_recv()
        w_core(n + 1).start()
    for p in range(5):
        for d in range(2):
            g_forward(p, d).wait_recv()
    def d_core(k):
        return send(dw_cs.at[k], dw_cr.at[k], dc_s.at[k], dc_r.at[k], core_dev)

    def d_x(n):
        return send(dw_xs.at[n], dw_xr.at[n], dxx_s.at[n], dxx_r.at[n], at(dx=n + 1))

    def d_z(n):
        return send(dw_zs.at[n], dw_zr.at[n], dz_s.at[n], dz_r.at[n], at(dl=n + 1))

    def d_swap():
        return send(dw_sw, dw_gr, dsw_s, dsw_r, swap_dev)

    def product(half, n):
        k = lax.rem(x + 1 + n, 4)
        rhs = g[:, :, :, lanes(k * COLS, COLS)].reshape(1024, COLS)
        return dot(xt[half], rhs, 1, 0)

    def for_core(n, _):
        dw_cs[n] = product(other_c, n).astype(BF)
        d_core(n).start()
        return 0

    def for_x(n, _):
        part = product(c, n)
        d_core(n).wait_recv()
        part = part + dw_cr[n].astype(F32)

        @pl.when(n < 3)
        def _():
            dw_xs[n] = part.astype(BF)
            d_x(n).start()

        @pl.when(n == 3)
        def _():
            dw_acc[...] = part

        return 0

    def e_z(n):
        to = lax.rem(y + 1 + min(n, 3), 4)
        rows = pl.ds(0, 128) if n < 3 else pl.ds((n - 3) * 64, 64)
        return send(dx_s.at[to, rows], dx_r.at[to, rows], ez_s.at[n], ez_r.at[n], zh_dev)

    def e_y(n):
        dst = gx_ref.at[0, :, lanes(y * 1024, 1024)]
        return send(dx_f.at[n], dst, ey_s.at[n], ey_r.at[n], at(dy=n + 1))

    def back(tokens, half):
        return dot(g[:, tokens].reshape(512, ALL), w[half], 1, 1)

    for n in range(4):
        w_core(n).wait()
    for half in range(2):
        r = back(other_zh, half).astype(BF).reshape(4, 128, 512)
        for b in range(4):
            dx_s[:, :, b * 256 + half * 128 : b * 256 + half * 128 + 128] = r[:, :, b * 128 : b * 128 + 128]
    for n in range(4):
        e_z(n).start()
    for n in range(4):
        x_z(n).wait_recv()
    lax.fori_loop(0, 4, lambda b, _: turn(2 * b + other_zh, 0), 0)
    lax.fori_loop(0, 4, for_core, 0)
    lax.fori_loop(0, 4, for_x, 0)

    for half in range(2):
        r = back(zh, half).reshape(4, 128, 512)
        for b in range(4):
            dx_o[:, :, b * 256 + half * 128 : b * 256 + half * 128 + 128] = r[:, :, b * 128 : b * 128 + 128]

    def finish(n):
        e_z(n).wait_recv()
        if n == 3:
            e_z(4).wait_recv()
        to = lax.rem(y + 1 + n, 4)
        done = (dx_o[to] + dx_r[to].astype(F32)).astype(BF)
        if n < 3:
            dx_f[n] = done
            e_y(n).start()
        else:
            gx_ref[0, :, lanes(y * 1024, 1024)] = done

    finish(0)
    finish(1)
    for n in range(3):
        d_x(n).wait_recv()

    def summed(rows):
        r = dw_acc[rows, :]
        for n in range(3):
            r = r + dw_xr[n, rows, :].astype(F32)
        return r

    for n in range(3):
        dw_zs[n] = summed(pl.ds(lax.rem(zl + n + 1, 4) * 128, 128)).astype(BF)
        d_z(n).start()
    dw_fin[...] = summed(pl.ds(zl * 128, 128))
    finish(2)
    for n in range(3):
        d_z(n).wait_recv()
    grad = dw_fin[...]
    for n in range(3):
        grad = grad + dw_zr[n].astype(F32)
    dw_sw[...] = grad.astype(BF)

    def s_plane(n):
        return send(sq2.at[0], sq2.at[n + 1], s2_s.at[n], s2_r.at[n], at(dx=plane[n][0], dy=plane[n][1]))

    def s_column(n):
        return send(sq1.at[0], sq1.at[n + 1], s1_s.at[n], s1_r.at[n], line(*column[n]))

    squares = jnp.sum((grad * grad).reshape(16, 8, COLS), axis=0)
    sq1[0] = sum(squares[:, b * 128 : b * 128 + 128] for b in range(5))
    for n in range(15):
        s_column(n).start()
    for n in range(15):
        s_column(n).wait_recv()
    sq2[0] = jnp.sum(sq1[...], axis=0)
    for n in range(15):
        s_plane(n).start()
    e_z(4).start()

    @pl.when(x != y)
    def _():
        d_swap().start()

    @pl.when(x == y)
    def _():
        dw_gr[...] = dw_sw[...]

    for n in range(15):
        s_plane(n).wait_recv()
    squared_total = jnp.sum(jnp.sum(sq2[...], axis=0), keepdims=True)
    entries = MODEL_FEATURES * (QUERY_HEADS + 2 * KEY_VALUE_HEADS) * HEAD
    factor = 1.0 / jnp.maximum(jnp.sqrt(squared_total / entries), 1.0)

    @pl.when(x != y)
    def _():
        d_swap().wait()

    for load in loads[4:]:
        load.wait()
    vq_ref[...] = 0.9 * mq_ref[...] + factor * dw_gr[:, :384].astype(F32)
    vk_ref[...] = 0.9 * mk_ref[...] + factor * dw_gr[:, 384:512].astype(F32)
    vv_ref[...] = 0.9 * mv_ref[...] + factor * dw_gr[:, 512:].astype(F32)
    finish(3)

    for n in range(3):
        e_y(n).wait()
        x_y(n).wait_send()
        d_x(n).wait_send()
        d_z(n).wait_send()
        w_near(n).wait_send()
        for m in range(4):
            w_far(m, n).wait_send()
    for n in range(4):
        x_z(n).wait_send()
        d_core(n).wait_send()
        e_z(n).wait_send()
    e_z(4).wait_send()
    for p in range(5):
        for d in range(2):
            g_own(p, d).wait_send()
            g_forward(p, d).wait_send()
    for n in range(15):
        s_plane(n).wait_send()
        s_column(n).wait_send()


def local(*args):
    vm = pltpu.VMEM
    scratch = [
        vm((1, 1024, 384), BF), vm((1, 1024, HEAD), BF), vm((1, 1024, HEAD), BF), vm((1, 1024, 384), BF),
        vm((128, 384), F32), vm((128, HEAD), F32), vm((128, HEAD), F32),
        pltpu.SemaphoreType.DMA((7,)), pltpu.SemaphoreType.DMA((3,)), pltpu.SemaphoreType.DMA,
        vm((1024, 1024), BF), vm((2, 512, 1024), BF), vm((4, 2, 128, ALL), BF), vm((2, 512, ALL), BF),
        vm((1024, QB), F32), vm((1024, QB), F32), vm((1024, QB), BF), vm((1024, QB), BF),
        vm((1024, HEAD), F32), vm((1024, HEAD), F32),
        vm((4, 512, COLS), BF), vm((4, 512, COLS), BF), vm((3, 512, COLS), BF), vm((3, 512, COLS), BF),
        vm((512, COLS), F32), vm((3, 128, COLS), BF), vm((3, 128, COLS), BF), vm((128, COLS), F32),
        vm((128, COLS), BF), vm((128, COLS), BF),
        vm((4, 128, 1024), BF), vm((4, 128, 1024), BF), vm((4, 128, 1024), F32), vm((3, 128, 1024), BF),
        vm((16, 8, 128), F32), vm((16, 8, 128), F32),
    ]
    shapes = [(3,), (3,), (4, 3), (4,), (3,), (4,), (2, 5), (2, 5), (4,), (3,), (3,), (), (5,), (3,), (15,), (15,)]
    for shape in shapes:
        scratch += [pltpu.SemaphoreType.DMA(shape)] * 2
    whole = pl.BlockSpec(memory_space=pltpu.VMEM)
    return pl.pallas_call(
        kernel,
        out_shape=(
            jax.ShapeDtypeStruct((1, 128, MODEL_FEATURES), BF),
            jax.ShapeDtypeStruct((128, 384), F32),
            jax.ShapeDtypeStruct((128, 128), F32),
            jax.ShapeDtypeStruct((128, 128), F32),
        ),
        in_specs=[pl.BlockSpec(memory_space=pltpu.HBM)] * 11,
        out_specs=(whole,) * 4,
        scratch_shapes=scratch,
        compiler_params=pltpu.CompilerParams(
            collective_id=0, has_side_effects=True, vmem_limit_bytes=62 * 1024 * 1024
        ),
        name="block",
    )(*args)


def solution(mesh):
    torus = Mesh(mesh.devices.reshape(4, 4, 2, 4, 2), AXES)
    in_specs = (
        P(DP, TENSOR, None),
        P(DP, None, TENSOR),
        P(DP, None, TENSOR),
        P(DP, None, TENSOR),
        P(DP, None, TENSOR),
        P(DP, TENSOR),
        P(DP, TENSOR),
        P(DP, TENSOR),
        P(DP, TENSOR),
        P(DP, TENSOR),
        P(DP, TENSOR),
    )
    out_specs = (P(DP, TENSOR, None), P(DP, TENSOR), P(DP, TENSOR), P(DP, TENSOR))
    return jax.shard_map(local, mesh=torus, in_specs=in_specs, out_specs=out_specs, check_vma=False)
```

```python
import functools
import math

import jax
import jax.numpy as jnp
from jax import lax
from jax.experimental import pallas as pl
from jax.experimental.pallas import tpu as pltpu
from jax.sharding import Mesh
from jax.sharding import PartitionSpec as P

MODEL_FEATURES = 4096
QUERY_HEADS = 24
KEY_VALUE_HEADS = 8
HEAD = 128
DP = ("dp_0", "dp_1", "dp_2")
TENSOR = ("tensor_0", "tensor_1")
AXES = DP + TENSOR
MESH = pl.DeviceIdType.MESH
BF = jnp.bfloat16
F32 = jnp.float32

COLS = 640
ALL = 4 * COLS
QB = 256


def dot(a, b, ca, cb):
    return lax.dot_general(a, b, (((ca,), (cb,)), ((), ())), preferred_element_type=F32)


def lanes(start, size):
    return pl.ds(pl.multiple_of(start, 128), size)


def kernel(
    in_ref, q_hbm, k_hbm, v_hbm, do_hbm, wq_ref, wk_ref, wv_ref, mq_hbm, mk_hbm, mv_hbm,
    gx_ref, vq_ref, vk_ref, vv_ref,
    q_ref, k_ref, v_ref, do_ref, mq_ref, mk_ref, mv_ref, l_sem, lw_sem, lx_sem,
    xq, xt, g, w, s_buf, dp_buf, p_buf, ds_buf, dk_acc, dv_acc,
    dw_cs, dw_cr, dw_xs, dw_xr, dw_vs, dw_vr, dw_h, dw_acc, dw_zs, dw_zr, dw_fin, dw_sw, dw_gr,
    dx_s, dx_r, dx_o, dx_f, sq1, sq2,
    ws_s, ws_r, wz_s, wz_r, wx_s, wx_r, wc_s, wc_r,
    xy_s, xy_r, xz_s, xz_r, go_s, go_r, gf_s, gf_r,
    dc_s, dc_r, dv_s, dv_r, dxx_s, dxx_r, dz_s, dz_r, dsw_s, dsw_r,
    ez_s, ez_r, ey_s, ey_r, s1_s, s1_r, s2_s, s2_r,
):
    x, zl, c, y, zh = (lax.axis_index(a) for a in AXES)
    scaling = 1.0 / math.sqrt(HEAD)
    other_c, other_zh = 1 - c, 1 - zh

    def at(dx=0, dl=0, dy=0):
        return (lax.rem(x + dx, 4), lax.rem(zl + dl, 4), c, lax.rem(y + dy, 4), zh)

    pair, across = zl + 1 - 2 * lax.rem(zl, 2), lax.rem(zl + 2, 4)
    blocks = (zl, across, pair, 3 - zl)
    pair_dev = (x, pair, c, y, zh)
    across_dev = (x, across, c, y, zh)
    swap_dev = (y, zl, c, x, zh)
    core_dev = (x, zl, other_c, y, zh)
    zh_dev = (x, zl, c, y, other_zh)

    def line(dz, dc):
        z = lax.rem(zh * 4 + zl + dz, 8)
        return (x, lax.rem(z, 4), lax.rem(c + dc, 2), y, z // 4)

    plane = [(dx, dy) for dx in range(4) for dy in range(4) if dx or dy]
    column = [(dz, dc) for dz in range(8) for dc in range(2) if dz or dc]

    def send(src, dst, ss, rs, dev):
        return pltpu.make_async_remote_copy(
            src_ref=src, dst_ref=dst, send_sem=ss, recv_sem=rs, device_id=dev, device_id_type=MESH
        )

    barrier = pltpu.get_barrier_semaphore()
    for dx, dy in plane:
        pl.semaphore_signal(barrier, inc=1, device_id=at(dx=dx, dy=dy), device_id_type=MESH)
    for dz, dc in column:
        pl.semaphore_signal(barrier, inc=1, device_id=line(dz, dc), device_id_type=MESH)
    loads = [
        pltpu.make_async_copy(src, dst, l_sem.at[n])
        for n, (src, dst) in enumerate(
            (
                (q_hbm, q_ref), (k_hbm, k_ref), (v_hbm, v_ref), (do_hbm, do_ref),
                (mq_hbm, mq_ref), (mk_hbm, mk_ref), (mv_hbm, mv_ref),
            )
        )
    ]
    for load in loads:
        load.start()
    pl.semaphore_wait(barrier, 30)

    w_rows = pl.ds(zl * 128, 128)
    w_parts = ((wq_ref, 0, 384), (wk_ref, 384, 128), (wv_ref, 512, 128))

    def w_swap(n):
        ref, off, size = w_parts[n]
        dst = w.at[c, w_rows, lanes(y * COLS + off, size)]
        return send(ref, dst, ws_s.at[n], ws_r.at[n], swap_dev)

    def w_here(n):
        ref, off, size = w_parts[n]
        return pltpu.make_async_copy(ref, w.at[c, w_rows, lanes(x * COLS + off, size)], lw_sem.at[n])

    def w_block(m):
        return w.at[c, pl.ds(blocks[m] * 128, 128), lanes(x * COLS, COLS)]

    def w_near(m):
        block = w_block((None, 0, 0, 1)[m])
        dev = across_dev if m == 1 else pair_dev
        return send(block, block, wz_s.at[m - 1], wz_r.at[m - 1], dev)

    def w_far(m, n):
        return send(w_block(m), w_block(m), wx_s.at[m, n], wx_r.at[m, n], at(dx=n + 1))

    def w_core(n):
        part = w.at[c, :, lanes(lax.rem(x + 4 - n, 4) * COLS, COLS)]
        return send(part, part, wc_s.at[n], wc_r.at[n], core_dev)

    @pl.when(x != y)
    def _():
        for n in range(3):
            w_swap(n).start()

    @pl.when(x == y)
    def _():
        for n in range(3):
            w_here(n).start()

    def x_rows(dy):
        return pl.ds((2 * lax.rem(y + 4 - dy, 4) + zh) * 128, 128)

    def x_y(n):
        to = lax.rem(y + n + 1, 4)
        return send(
            in_ref.at[0, :, lanes(to * 1024, 1024)], xq.at[x_rows(0)],
            xy_s.at[n], xy_r.at[n], at(dy=n + 1),
        )

    def x_z(n):
        rows = xq.at[x_rows(n)]
        return send(rows, rows, xz_s.at[n], xz_r.at[n], zh_dev)

    own_x = in_ref.at[0, :, lanes(y * 1024, 1024)]
    send(own_x, xq.at[x_rows(0)], xz_s.at[0], xz_r.at[0], zh_dev).start()
    for n in range(3):
        x_y(n).start()
    x_here = pltpu.make_async_copy(own_x, xq.at[x_rows(0)], lx_sem)
    x_here.start()
    for load in loads[:4]:
        load.wait()

    def g_own(p, d):
        piece = g.at[:, :, :, lanes(y * COLS + p * 128, 128)]
        return send(piece, piece, go_s.at[d, p], go_r.at[d, p], at(dy=1 if d == 0 else 3))

    def g_forward(p, d):
        of = lax.rem(y + (3 if d == 0 else 1), 4)
        half = g.at[2 * d : 2 * d + 2, :, :, lanes(of * COLS + p * 128, 128)]
        return send(half, half, gf_s.at[d, p], gf_r.at[d, p], at(dy=1 if d == 0 else 3))

    dk_acc[...] = jnp.zeros_like(dk_acc)
    dv_acc[...] = jnp.zeros_like(dv_acc)
    causal = lax.broadcasted_iota(jnp.int32, (QB, QB), 0) <= lax.broadcasted_iota(
        jnp.int32, (QB, QB), 1
    )

    def head(h, _):
        cols = lanes(h * HEAD, HEAD)
        for i in range(4):
            rows = pl.ds(i * QB, QB)
            qi, doi = q_ref[0, rows, cols], do_ref[0, rows, cols]
            width = (i + 1) * QB
            top = None
            for j in range(i + 1):
                js = pl.ds(j * QB, QB)
                s = dot(k_ref[0, js, :], qi, 1, 1) * scaling
                if j == i:
                    s = jnp.where(causal, s, -jnp.inf)
                s_buf[js, :] = s
                m = jnp.max(s, axis=0, keepdims=True)
                top = m if top is None else jnp.maximum(top, m)
            total = jnp.zeros((1, QB), F32)
            delta = jnp.zeros((1, QB), F32)
            for j in range(i + 1):
                js = pl.ds(j * QB, QB)
                e = jnp.exp(s_buf[js, :] - top)
                dp = dot(v_ref[0, js, :], doi, 1, 1)
                s_buf[js, :] = e
                dp_buf[js, :] = dp
                total = total + jnp.sum(e, axis=0, keepdims=True)
                delta = delta + jnp.sum(e * dp, axis=0, keepdims=True)
            inverse = 1.0 / total
            delta = delta * inverse
            for j in range(i + 1):
                js = pl.ds(j * QB, QB)
                p = s_buf[js, :] * inverse
                p_buf[js, :] = p.astype(BF)
                ds_buf[js, :] = (p * (dp_buf[js, :] - delta) * scaling).astype(BF)
            dv_acc[:width, :] += dot(p_buf[:width, :], doi, 1, 0)
            dk_acc[:width, :] += dot(ds_buf[:width, :], qi, 1, 0)
            dq = dot(ds_buf[:width, :], k_ref[0, :width, :], 0, 0).astype(BF)
            g[i, :, :, lanes(y * COLS + h * HEAD, HEAD)] = dq.reshape(2, 128, HEAD)
        @pl.when(h == 0)
        def _():
            @pl.when(x != y)
            def _():
                for n in range(3):
                    w_swap(n).wait()

            @pl.when(x == y)
            def _():
                for n in range(3):
                    w_here(n).wait()

            w_near(1).start()
            w_near(2).start()
            for n in range(3):
                w_far(0, n).start()

        g_own(h, 0).start()
        g_own(h, 1).start()
        return 0

    lax.fori_loop(0, 3, head, 0)
    for p, acc in ((3, dk_acc), (4, dv_acc)):
        g[:, :, :, lanes(y * COLS + p * 128, 128)] = acc[...].astype(BF).reshape(4, 2, 128, 128)
        g_own(p, 0).start()
        g_own(p, 1).start()

    def turn(t, _):
        rows = pl.ds(pl.multiple_of(t * 128, 128), 128)
        for b in range(8):
            block = xq[rows, b * 128 : b * 128 + 128]
            xt[b % 2, (b // 2) * 128 : (b // 2) * 128 + 128, lanes(t * 128, 128)] = block.T
        return 0

    def forward(p):
        for d in range(2):
            g_own(p, d).wait_recv()
            g_forward(p, d).start()

    def spread(m):
        w_near(m).wait_recv()
        if m == 1:
            w_near(3).start()
        for n in range(3):
            w_far(m, n).start()

    spread(1)
    for n in range(3):
        x_y(n).wait_recv()
    spread(2)
    for n in range(3):
        x_z(n + 1).start()
    forward(0)
    forward(1)
    spread(3)
    w_core(0).start()
    forward(2)
    forward(3)
    forward(4)
    x_here.wait()
    lax.fori_loop(0, 4, lambda b, _: turn(2 * b + zh, 0), 0)
    def d_core(j):
        return send(dw_cs.at[j], dw_cr.at[j], dc_s.at[j], dc_r.at[j], core_dev)

    def d_x(d, half):
        rows = pl.ds(256 * half, 256)
        return send(
            dw_xs.at[d, rows], dw_xr.at[d, rows], dxx_s.at[d, half], dxx_r.at[d, half],
            at(dx=1 if d == 0 else 3),
        )

    def d_via(d):
        return send(dw_vs.at[d], dw_vr.at[d], dv_s.at[d], dv_r.at[d], at(dx=1 if d == 0 else 3))

    def d_z(n):
        dev = across_dev if n == 2 else pair_dev
        return send(dw_zs.at[n], dw_zr.at[n], dz_s.at[n], dz_r.at[n], dev)

    def d_swap():
        return send(dw_sw, dw_gr, dsw_s, dsw_r, swap_dev)

    def product(half, k):
        rhs = g[:, :, :, lanes(k * COLS, COLS)].reshape(1024, COLS)
        return dot(xt[half], rhs, 1, 0)

    def for_core(j):
        dw_cs[j] = product(other_c, lax.rem(y + j, 4)).astype(BF)
        d_core(j).start()

    def for_x(n):
        k = lax.rem(x + n, 4)
        j = lax.rem(k + 4 - y, 4)
        part = product(c, k)
        d_core(j).wait_recv()
        return part + dw_cr[j].astype(F32)

    def e_z(n):
        to = lax.rem(y + 1 + min(n, 3), 4)
        rows = pl.ds(0, 128) if n < 3 else pl.ds((n - 3) * 64, 64)
        return send(dx_s.at[to, rows], dx_r.at[to, rows], ez_s.at[n], ez_r.at[n], zh_dev)

    def e_y(n):
        dst = gx_ref.at[0, :, lanes(y * 1024, 1024)]
        return send(dx_f.at[n], dst, ey_s.at[n], ey_r.at[n], at(dy=n + 1))

    def back(tokens, half):
        return dot(g[:, tokens].reshape(512, ALL), w[half], 1, 1)

    for n in range(3):
        for m in range(4):
            w_far(m, n).wait_recv()
        w_core(n + 1).start()
    for n in range(4):
        x_z(n).wait_recv()
    lax.fori_loop(0, 4, lambda b, _: turn(2 * b + other_zh, 0), 0)
    for j in (0, 1, 3):
        for_core(j)
    for p in range(5):
        for d in range(2):
            g_forward(p, d).wait_recv()
    for_core(2)
    for n in range(4):
        w_core(n).wait()
    for half in range(2):
        r = back(other_zh, half).astype(BF).reshape(4, 128, 512)
        for b in range(4):
            dx_s[:, :, b * 256 + half * 128 : b * 256 + half * 128 + 128] = r[:, :, b * 128 : b * 128 + 128]
    for n in range(4):
        e_z(n).start()
    far = for_x(2)
    for d in range(2):
        dw_vs[d] = far[256 * d : 256 * d + 256].astype(BF)
        d_via(d).start()
    for d in range(2):
        near = for_x(1 if d == 0 else 3)
        dw_xs[d, pl.ds(256 * (1 - d), 256)] = near[256 * (1 - d) : 256 * (1 - d) + 256].astype(BF)
        d_x(d, 1 - d).start()
        dw_h[d] = near[256 * d : 256 * d + 256]
    dw_acc[...] = for_x(0)
    for half in range(2):
        r = back(zh, half).reshape(4, 128, 512)
        for b in range(4):
            dx_o[:, :, b * 256 + half * 128 : b * 256 + half * 128 + 128] = r[:, :, b * 128 : b * 128 + 128]

    def finish(n):
        e_z(n).wait_recv()
        if n == 3:
            e_z(4).wait_recv()
        to = lax.rem(y + 1 + n, 4)
        done = (dx_o[to] + dx_r[to].astype(F32)).astype(BF)
        if n < 3:
            dx_f[n] = done
            e_y(n).start()
        else:
            gx_ref[0, :, lanes(y * 1024, 1024)] = done

    for d in range(2):
        d_via(d).wait_recv()
        dw_xs[d, pl.ds(256 * d, 256)] = (dw_h[d] + dw_vr[d].astype(F32)).astype(BF)
        d_x(d, d).start()
    finish(0)
    finish(1)
    for d in range(2):
        for half in range(2):
            d_x(d, half).wait_recv()

    def summed(rows):
        r = dw_acc[rows, :]
        for d in range(2):
            r = r + dw_xr[d, rows, :].astype(F32)
        return r

    for n, to in ((1, 3), (0, 2)):
        dw_zs[n] = summed(pl.ds(blocks[to] * 128, 128)).astype(BF)
        d_z(n).start()
    rest = summed(pl.ds(across * 128, 128))
    d_z(1).wait_recv()
    dw_zs[2] = (rest + dw_zr[1].astype(F32)).astype(BF)
    d_z(2).start()
    dw_fin[...] = summed(pl.ds(zl * 128, 128))
    finish(2)
    d_z(0).wait_recv()
    d_z(2).wait_recv()
    grad = dw_fin[...] + dw_zr[0].astype(F32) + dw_zr[2].astype(F32)
    dw_sw[...] = grad.astype(BF)

    @pl.when(x != y)
    def _():
        d_swap().start()

    @pl.when(x == y)
    def _():
        dw_gr[...] = dw_sw[...]

    def s_plane(n):
        return send(sq2.at[0], sq2.at[n + 1], s2_s.at[n], s2_r.at[n], at(dx=plane[n][0], dy=plane[n][1]))

    def s_column(n):
        return send(sq1.at[0], sq1.at[n + 1], s1_s.at[n], s1_r.at[n], line(*column[n]))

    squares = jnp.sum((grad * grad).reshape(16, 8, COLS), axis=0)
    sq1[0] = sum(squares[:, b * 128 : b * 128 + 128] for b in range(5))
    for n in range(15):
        s_column(n).start()
    for n in range(15):
        s_column(n).wait_recv()
    sq2[0] = jnp.sum(sq1[...], axis=0)
    for n in range(15):
        s_plane(n).start()
    e_z(4).start()

    for n in range(15):
        s_plane(n).wait_recv()
    squared_total = jnp.sum(jnp.sum(sq2[...], axis=0), keepdims=True)
    entries = MODEL_FEATURES * (QUERY_HEADS + 2 * KEY_VALUE_HEADS) * HEAD
    factor = 1.0 / jnp.maximum(jnp.sqrt(squared_total / entries), 1.0)

    @pl.when(x != y)
    def _():
        d_swap().wait()

    for load in loads[4:]:
        load.wait()
    vq_ref[...] = 0.9 * mq_ref[...] + factor * dw_gr[:, :384].astype(F32)
    vk_ref[...] = 0.9 * mk_ref[...] + factor * dw_gr[:, 384:512].astype(F32)
    vv_ref[...] = 0.9 * mv_ref[...] + factor * dw_gr[:, 512:].astype(F32)
    finish(3)

    for n in range(3):
        e_y(n).wait()
        x_y(n).wait_send()
        d_z(n).wait_send()
        w_near(n + 1).wait_send()
        for m in range(4):
            w_far(m, n).wait_send()
    for n in range(4):
        x_z(n).wait_send()
        d_core(n).wait_send()
        e_z(n).wait_send()
    e_z(4).wait_send()
    for d in range(2):
        d_via(d).wait_send()
        for half in range(2):
            d_x(d, half).wait_send()
    for p in range(5):
        for d in range(2):
            g_own(p, d).wait_send()
            g_forward(p, d).wait_send()
    for n in range(15):
        s_plane(n).wait_send()
        s_column(n).wait_send()


def local(*args):
    vm = pltpu.VMEM
    scratch = [
        vm((1, 1024, 384), BF), vm((1, 1024, HEAD), BF), vm((1, 1024, HEAD), BF), vm((1, 1024, 384), BF),
        vm((128, 384), F32), vm((128, HEAD), F32), vm((128, HEAD), F32),
        pltpu.SemaphoreType.DMA((7,)), pltpu.SemaphoreType.DMA((3,)), pltpu.SemaphoreType.DMA,
        vm((1024, 1024), BF), vm((2, 512, 1024), BF), vm((4, 2, 128, ALL), BF), vm((2, 512, ALL), BF),
        vm((1024, QB), F32), vm((1024, QB), F32), vm((1024, QB), BF), vm((1024, QB), BF),
        vm((1024, HEAD), F32), vm((1024, HEAD), F32),
        vm((4, 512, COLS), BF), vm((4, 512, COLS), BF), vm((2, 512, COLS), BF), vm((2, 512, COLS), BF),
        vm((2, 256, COLS), BF), vm((2, 256, COLS), BF), vm((2, 256, COLS), F32),
        vm((512, COLS), F32), vm((3, 128, COLS), BF), vm((3, 128, COLS), BF), vm((128, COLS), F32),
        vm((128, COLS), BF), vm((128, COLS), BF),
        vm((4, 128, 1024), BF), vm((4, 128, 1024), BF), vm((4, 128, 1024), F32), vm((3, 128, 1024), BF),
        vm((16, 8, 128), F32), vm((16, 8, 128), F32),
    ]
    shapes = [(3,), (3,), (4, 3), (4,), (3,), (4,), (2, 5), (2, 5), (4,), (2,), (2, 2), (3,), (), (5,), (3,), (15,), (15,)]
    for shape in shapes:
        scratch += [pltpu.SemaphoreType.DMA(shape)] * 2
    whole = pl.BlockSpec(memory_space=pltpu.VMEM)
    return pl.pallas_call(
        kernel,
        out_shape=(
            jax.ShapeDtypeStruct((1, 128, MODEL_FEATURES), BF),
            jax.ShapeDtypeStruct((128, 384), F32),
            jax.ShapeDtypeStruct((128, 128), F32),
            jax.ShapeDtypeStruct((128, 128), F32),
        ),
        in_specs=[pl.BlockSpec(memory_space=pltpu.HBM)] * 11,
        out_specs=(whole,) * 4,
        scratch_shapes=scratch,
        compiler_params=pltpu.CompilerParams(
            collective_id=0, has_side_effects=True, vmem_limit_bytes=62 * 1024 * 1024
        ),
        name="block",
    )(*args)


def solution(mesh):
    torus = Mesh(mesh.devices.reshape(4, 4, 2, 4, 2), AXES)
    in_specs = (
        P(DP, TENSOR, None),
        P(DP, None, TENSOR),
        P(DP, None, TENSOR),
        P(DP, None, TENSOR),
        P(DP, None, TENSOR),
        P(DP, TENSOR),
        P(DP, TENSOR),
        P(DP, TENSOR),
        P(DP, TENSOR),
        P(DP, TENSOR),
        P(DP, TENSOR),
    )
    out_specs = (P(DP, TENSOR, None), P(DP, TENSOR), P(DP, TENSOR), P(DP, TENSOR))
    return jax.shard_map(local, mesh=torus, in_specs=in_specs, out_specs=out_specs, check_vma=False)
```

```python
import functools
import math

import jax
import jax.numpy as jnp
from jax import lax
from jax.experimental import pallas as pl
from jax.experimental.pallas import tpu as pltpu
from jax.sharding import Mesh
from jax.sharding import PartitionSpec as P

MODEL_FEATURES = 4096
QUERY_HEADS = 24
KEY_VALUE_HEADS = 8
HEAD = 128
DP = ("dp_0", "dp_1", "dp_2")
TENSOR = ("tensor_0", "tensor_1")
AXES = DP + TENSOR
MESH = pl.DeviceIdType.MESH
BF = jnp.bfloat16
F32 = jnp.float32

COLS = 640
ALL = 4 * COLS
QB = 256


def dot(a, b, ca, cb):
    return lax.dot_general(a, b, (((ca,), (cb,)), ((), ())), preferred_element_type=F32)


def lanes(start, size):
    return pl.ds(pl.multiple_of(start, 128), size)


def kernel(
    in_ref, q_hbm, k_hbm, v_hbm, do_hbm, wq_ref, wk_ref, wv_ref, mq_hbm, mk_hbm, mv_hbm,
    gx_ref, vq_ref, vk_ref, vv_ref,
    q_ref, k_ref, v_ref, do_ref, mq_ref, mk_ref, mv_ref, l_sem, lw_sem, lx_sem,
    xq, xt, g, w, s_buf, dp_buf, p_buf, ds_buf, dk_acc, dv_acc,
    dw_cs, dw_cr, dw_xs, dw_xr, dw_vs, dw_vr, dw_h, dw_acc, dw_zs, dw_zr, dw_fin, dw_sw, dw_gr,
    dx_s, dx_r, dx_o, dx_f, sq1, sq2,
    ws_s, ws_r, wz_s, wz_r, wx_s, wx_r, wc_s, wc_r,
    xy_s, xy_r, xz_s, xz_r, go_s, go_r, gf_s, gf_r,
    dc_s, dc_r, dv_s, dv_r, dxx_s, dxx_r, dz_s, dz_r, dsw_s, dsw_r,
    ez_s, ez_r, ey_s, ey_r, s1_s, s1_r, s2_s, s2_r,
):
    x, zl, c, y, zh = (lax.axis_index(a) for a in AXES)
    scaling = 1.0 / math.sqrt(HEAD)
    other_c, other_zh = 1 - c, 1 - zh

    def at(dx=0, dl=0, dy=0):
        return (lax.rem(x + dx, 4), lax.rem(zl + dl, 4), c, lax.rem(y + dy, 4), zh)

    pair, across = zl + 1 - 2 * lax.rem(zl, 2), lax.rem(zl + 2, 4)
    blocks = (zl, across, pair, 3 - zl)
    pair_dev = (x, pair, c, y, zh)
    across_dev = (x, across, c, y, zh)
    swap_dev = (y, zl, c, x, zh)
    core_dev = (x, zl, other_c, y, zh)
    zh_dev = (x, zl, c, y, other_zh)

    def line(dz, dc):
        z = lax.rem(zh * 4 + zl + dz, 8)
        return (x, lax.rem(z, 4), lax.rem(c + dc, 2), y, z // 4)

    plane = [(dx, dy) for dx in range(4) for dy in range(4) if dx or dy]
    column = [(dz, dc) for dz in range(8) for dc in range(2) if dz or dc]

    def send(src, dst, ss, rs, dev):
        return pltpu.make_async_remote_copy(
            src_ref=src, dst_ref=dst, send_sem=ss, recv_sem=rs, device_id=dev, device_id_type=MESH
        )

    barrier = pltpu.get_barrier_semaphore()
    for dx, dy in plane:
        pl.semaphore_signal(barrier, inc=1, device_id=at(dx=dx, dy=dy), device_id_type=MESH)
    for dz, dc in column:
        pl.semaphore_signal(barrier, inc=1, device_id=line(dz, dc), device_id_type=MESH)
    loads = [
        pltpu.make_async_copy(src, dst, l_sem.at[n])
        for n, (src, dst) in enumerate(
            (
                (q_hbm, q_ref), (k_hbm, k_ref), (v_hbm, v_ref), (do_hbm, do_ref),
                (mq_hbm, mq_ref), (mk_hbm, mk_ref), (mv_hbm, mv_ref),
            )
        )
    ]
    for load in loads:
        load.start()
    pl.semaphore_wait(barrier, 30)

    w_rows = pl.ds(zl * 128, 128)
    w_parts = ((wq_ref, 0, 384), (wk_ref, 384, 128), (wv_ref, 512, 128))

    def w_swap(n):
        ref, off, size = w_parts[n]
        dst = w.at[c, w_rows, lanes(y * COLS + off, size)]
        return send(ref, dst, ws_s.at[n], ws_r.at[n], swap_dev)

    def w_here(n):
        ref, off, size = w_parts[n]
        return pltpu.make_async_copy(ref, w.at[c, w_rows, lanes(x * COLS + off, size)], lw_sem.at[n])

    def w_block(m):
        return w.at[c, pl.ds(blocks[m] * 128, 128), lanes(x * COLS, COLS)]

    def w_near(m):
        block = w_block((None, 0, 0, 1)[m])
        dev = across_dev if m == 1 else pair_dev
        return send(block, block, wz_s.at[m - 1], wz_r.at[m - 1], dev)

    def w_far(m, n):
        return send(w_block(m), w_block(m), wx_s.at[m, n], wx_r.at[m, n], at(dx=n + 1))

    def w_core(n):
        part = w.at[c, :, lanes(lax.rem(x + 4 - n, 4) * COLS, COLS)]
        return send(part, part, wc_s.at[n], wc_r.at[n], core_dev)

    @pl.when(x != y)
    def _():
        for n in range(3):
            w_swap(n).start()

    @pl.when(x == y)
    def _():
        for n in range(3):
            w_here(n).start()

    def x_rows(dy):
        return pl.ds((2 * lax.rem(y + 4 - dy, 4) + zh) * 128, 128)

    def x_y(n):
        to = lax.rem(y + n + 1, 4)
        return send(
            in_ref.at[0, :, lanes(to * 1024, 1024)], xq.at[x_rows(0)],
            xy_s.at[n], xy_r.at[n], at(dy=n + 1),
        )

    def x_z(n):
        rows = xq.at[x_rows(n)]
        return send(rows, rows, xz_s.at[n], xz_r.at[n], zh_dev)

    own_x = in_ref.at[0, :, lanes(y * 1024, 1024)]
    send(own_x, xq.at[x_rows(0)], xz_s.at[0], xz_r.at[0], zh_dev).start()
    for n in range(3):
        x_y(n).start()
    x_here = pltpu.make_async_copy(own_x, xq.at[x_rows(0)], lx_sem)
    x_here.start()
    for load in loads[:4]:
        load.wait()

    def g_own(t, p, d):
        piece = g.at[:, (other_zh, zh)[t], :, lanes(y * COLS + p * 128, 128)]
        return send(piece, piece, go_s.at[t, d, p], go_r.at[t, d, p], at(dy=1 if d == 0 else 3))

    def g_forward(t, p, d):
        of = lax.rem(y + (3 if d == 0 else 1), 4)
        half = g.at[2 * d : 2 * d + 2, (other_zh, zh)[t], :, lanes(of * COLS + p * 128, 128)]
        return send(half, half, gf_s.at[t, d, p], gf_r.at[t, d, p], at(dy=1 if d == 0 else 3))

    dk_acc[...] = jnp.zeros_like(dk_acc)
    dv_acc[...] = jnp.zeros_like(dv_acc)
    causal = lax.broadcasted_iota(jnp.int32, (QB, QB), 0) <= lax.broadcasted_iota(
        jnp.int32, (QB, QB), 1
    )

    def head(h, _):
        cols = lanes(h * HEAD, HEAD)
        for i in range(4):
            rows = pl.ds(i * QB, QB)
            qi, doi = q_ref[0, rows, cols], do_ref[0, rows, cols]
            width = (i + 1) * QB
            top = None
            for j in range(i + 1):
                js = pl.ds(j * QB, QB)
                s = dot(k_ref[0, js, :], qi, 1, 1) * scaling
                if j == i:
                    s = jnp.where(causal, s, -jnp.inf)
                s_buf[js, :] = s
                m = jnp.max(s, axis=0, keepdims=True)
                top = m if top is None else jnp.maximum(top, m)
            total = jnp.zeros((1, QB), F32)
            delta = jnp.zeros((1, QB), F32)
            for j in range(i + 1):
                js = pl.ds(j * QB, QB)
                e = jnp.exp(s_buf[js, :] - top)
                dp = dot(v_ref[0, js, :], doi, 1, 1)
                s_buf[js, :] = e
                dp_buf[js, :] = dp
                total = total + jnp.sum(e, axis=0, keepdims=True)
                delta = delta + jnp.sum(e * dp, axis=0, keepdims=True)
            inverse = 1.0 / total
            delta = delta * inverse
            for j in range(i + 1):
                js = pl.ds(j * QB, QB)
                p = s_buf[js, :] * inverse
                p_buf[js, :] = p.astype(BF)
                ds_buf[js, :] = (p * (dp_buf[js, :] - delta) * scaling).astype(BF)
            dv_acc[:width, :] += dot(p_buf[:width, :], doi, 1, 0)
            dk_acc[:width, :] += dot(ds_buf[:width, :], qi, 1, 0)
            dq = dot(ds_buf[:width, :], k_ref[0, :width, :], 0, 0).astype(BF)
            g[i, :, :, lanes(y * COLS + h * HEAD, HEAD)] = dq.reshape(2, 128, HEAD)
        @pl.when(h == 0)
        def _():
            @pl.when(x != y)
            def _():
                for n in range(3):
                    w_swap(n).wait()

            @pl.when(x == y)
            def _():
                for n in range(3):
                    w_here(n).wait()

            w_near(1).start()
            w_near(2).start()
            for n in range(3):
                w_far(0, n).start()

        g_own(0, h, 0).start()
        g_own(0, h, 1).start()
        return 0

    lax.fori_loop(0, 3, head, 0)
    for p, acc in ((3, dk_acc), (4, dv_acc)):
        g[:, :, :, lanes(y * COLS + p * 128, 128)] = acc[...].astype(BF).reshape(4, 2, 128, 128)
        g_own(0, p, 0).start()
        g_own(0, p, 1).start()

    def turn(t, _):
        rows = pl.ds(pl.multiple_of(t * 128, 128), 128)
        for b in range(8):
            block = xq[rows, b * 128 : b * 128 + 128]
            xt[b % 2, (b // 2) * 128 : (b // 2) * 128 + 128, lanes(t * 128, 128)] = block.T
        return 0

    def forward(t, p):
        for d in range(2):
            g_own(t, p, d).wait_recv()
            g_forward(t, p, d).start()

    def spread(m):
        w_near(m).wait_recv()
        if m == 1:
            w_near(3).start()
        for n in range(3):
            w_far(m, n).start()

    spread(1)
    for n in range(3):
        x_y(n).wait_recv()
    spread(2)
    for n in range(3):
        x_z(n + 1).start()
    for p in range(5):
        forward(0, p)
    for p in range(5):
        for d in range(2):
            g_own(1, p, d).start()
    spread(3)
    w_core(0).start()
    x_here.wait()
    lax.fori_loop(0, 4, lambda b, _: turn(2 * b + zh, 0), 0)
    def d_core(j):
        return send(dw_cs.at[j], dw_cr.at[j], dc_s.at[j], dc_r.at[j], core_dev)

    def d_x(d, half):
        rows = pl.ds(256 * half, 256)
        return send(
            dw_xs.at[d, rows], dw_xr.at[d, rows], dxx_s.at[d, half], dxx_r.at[d, half],
            at(dx=1 if d == 0 else 3),
        )

    def d_via(d):
        return send(dw_vs.at[d], dw_vr.at[d], dv_s.at[d], dv_r.at[d], at(dx=1 if d == 0 else 3))

    def d_z(n):
        dev = across_dev if n == 2 else pair_dev
        return send(dw_zs.at[n], dw_zr.at[n], dz_s.at[n], dz_r.at[n], dev)

    def d_swap():
        return send(dw_sw, dw_gr, dsw_s, dsw_r, swap_dev)

    def product(half, k):
        rhs = g[:, :, :, lanes(k * COLS, COLS)].reshape(1024, COLS)
        return dot(xt[half], rhs, 1, 0)

    def for_core(j):
        dw_cs[j] = product(other_c, lax.rem(y + j, 4)).astype(BF)
        d_core(j).start()

    def for_x(n):
        k = lax.rem(x + n, 4)
        j = lax.rem(k + 4 - y, 4)
        part = product(c, k)
        d_core(j).wait_recv()
        return part + dw_cr[j].astype(F32)

    def e_z(q):
        to, rows = lax.rem(y + 1 + q // 2, 4), pl.ds((q % 2) * 64, 64)
        return send(dx_s.at[to, rows], dx_r.at[to, rows], ez_s.at[q], ez_r.at[q], zh_dev)

    def e_y(q):
        rows = pl.ds((q % 2) * 64, 64)
        dst = gx_ref.at[0, rows, lanes(y * 1024, 1024)]
        return send(dx_f.at[q // 2, rows], dst, ey_s.at[q], ey_r.at[q], at(dy=q // 2 + 1))

    def back(tokens, half):
        return dot(g[:, tokens].reshape(512, ALL), w[half], 1, 1)

    for p in range(3):
        forward(1, p)
    for n in range(3):
        for m in range(4):
            w_far(m, n).wait_recv()
        w_core(n + 1).start()
    forward(1, 3)
    forward(1, 4)
    for p in range(5):
        for d in range(2):
            g_forward(0, p, d).wait_recv()
    for n in range(4):
        w_core(n).wait()
    for half in range(2):
        r = back(other_zh, half).astype(BF).reshape(4, 128, 512)
        for b in range(4):
            dx_s[:, :, b * 256 + half * 128 : b * 256 + half * 128 + 128] = r[:, :, b * 128 : b * 128 + 128]
    for q in range(4):
        e_z(q).start()
    for n in range(4):
        x_z(n).wait_recv()
    lax.fori_loop(0, 4, lambda b, _: turn(2 * b + other_zh, 0), 0)
    for j in (0, 1, 3):
        for_core(j)
    for p in range(5):
        for d in range(2):
            g_forward(1, p, d).wait_recv()
    for_core(2)
    far = for_x(2)
    for d in range(2):
        dw_vs[d] = far[256 * d : 256 * d + 256].astype(BF)
        d_via(d).start()
    for d in range(2):
        near = for_x(1 if d == 0 else 3)
        dw_xs[d, pl.ds(256 * (1 - d), 256)] = near[256 * (1 - d) : 256 * (1 - d) + 256].astype(BF)
        d_x(d, 1 - d).start()
        dw_h[d] = near[256 * d : 256 * d + 256]
    dw_acc[...] = for_x(0)
    for half in range(2):
        r = back(zh, half).reshape(4, 128, 512)
        for b in range(4):
            dx_o[:, :, b * 256 + half * 128 : b * 256 + half * 128 + 128] = r[:, :, b * 128 : b * 128 + 128]

    def finish(q):
        e_z(q).wait_recv()
        to, rows = lax.rem(y + 1 + q // 2, 4), pl.ds((q % 2) * 64, 64)
        done = (dx_o[to, rows] + dx_r[to, rows].astype(F32)).astype(BF)
        if q < 6:
            dx_f[q // 2, rows] = done
            e_y(q).start()
        else:
            gx_ref[0, rows, lanes(y * 1024, 1024)] = done

    for d in range(2):
        d_via(d).wait_recv()
        dw_xs[d, pl.ds(256 * d, 256)] = (dw_h[d] + dw_vr[d].astype(F32)).astype(BF)
        d_x(d, d).start()
    e_z(4).start()
    e_z(5).start()
    for q in range(4):
        finish(q)
    for d in range(2):
        for half in range(2):
            d_x(d, half).wait_recv()

    def summed(rows):
        r = dw_acc[rows, :]
        for d in range(2):
            r = r + dw_xr[d, rows, :].astype(F32)
        return r

    for n, to in ((1, 3), (0, 2)):
        dw_zs[n] = summed(pl.ds(blocks[to] * 128, 128)).astype(BF)
        d_z(n).start()
    rest = summed(pl.ds(across * 128, 128))
    d_z(1).wait_recv()
    dw_zs[2] = (rest + dw_zr[1].astype(F32)).astype(BF)
    d_z(2).start()
    dw_fin[...] = summed(pl.ds(zl * 128, 128))
    finish(4)
    finish(5)
    d_z(0).wait_recv()
    d_z(2).wait_recv()
    grad = dw_fin[...] + dw_zr[0].astype(F32) + dw_zr[2].astype(F32)
    dw_sw[...] = grad.astype(BF)

    @pl.when(x != y)
    def _():
        d_swap().start()

    @pl.when(x == y)
    def _():
        dw_gr[...] = dw_sw[...]

    def s_plane(n):
        return send(sq2.at[0], sq2.at[n + 1], s2_s.at[n], s2_r.at[n], at(dx=plane[n][0], dy=plane[n][1]))

    def s_column(n):
        return send(sq1.at[0], sq1.at[n + 1], s1_s.at[n], s1_r.at[n], line(*column[n]))

    squares = jnp.sum((grad * grad).reshape(16, 8, COLS), axis=0)
    sq1[0] = sum(squares[:, b * 128 : b * 128 + 128] for b in range(5))
    for n in range(15):
        s_column(n).start()
    e_z(6).start()
    e_z(7).start()
    for n in range(15):
        s_column(n).wait_recv()
    sq2[0] = jnp.sum(sq1[...], axis=0)
    for n in range(15):
        s_plane(n).start()

    for n in range(15):
        s_plane(n).wait_recv()
    squared_total = jnp.sum(jnp.sum(sq2[...], axis=0), keepdims=True)
    entries = MODEL_FEATURES * (QUERY_HEADS + 2 * KEY_VALUE_HEADS) * HEAD
    factor = 1.0 / jnp.maximum(jnp.sqrt(squared_total / entries), 1.0)

    @pl.when(x != y)
    def _():
        d_swap().wait()

    for load in loads[4:]:
        load.wait()
    vq_ref[...] = 0.9 * mq_ref[...] + factor * dw_gr[:, :384].astype(F32)
    vk_ref[...] = 0.9 * mk_ref[...] + factor * dw_gr[:, 384:512].astype(F32)
    vv_ref[...] = 0.9 * mv_ref[...] + factor * dw_gr[:, 512:].astype(F32)
    finish(6)
    finish(7)

    for n in range(3):
        x_y(n).wait_send()
        d_z(n).wait_send()
        w_near(n + 1).wait_send()
        for m in range(4):
            w_far(m, n).wait_send()
    for n in range(4):
        x_z(n).wait_send()
        d_core(n).wait_send()
    for q in range(8):
        e_z(q).wait_send()
    for q in range(6):
        e_y(q).wait()
    for d in range(2):
        d_via(d).wait_send()
        for half in range(2):
            d_x(d, half).wait_send()
    for p in range(5):
        for d in range(2):
            for t in range(2):
                g_own(t, p, d).wait_send()
                g_forward(t, p, d).wait_send()
    for n in range(15):
        s_plane(n).wait_send()
        s_column(n).wait_send()


def local(*args):
    vm = pltpu.VMEM
    scratch = [
        vm((1, 1024, 384), BF), vm((1, 1024, HEAD), BF), vm((1, 1024, HEAD), BF), vm((1, 1024, 384), BF),
        vm((128, 384), F32), vm((128, HEAD), F32), vm((128, HEAD), F32),
        pltpu.SemaphoreType.DMA((7,)), pltpu.SemaphoreType.DMA((3,)), pltpu.SemaphoreType.DMA,
        vm((1024, 1024), BF), vm((2, 512, 1024), BF), vm((4, 2, 128, ALL), BF), vm((2, 512, ALL), BF),
        vm((1024, QB), F32), vm((1024, QB), F32), vm((1024, QB), BF), vm((1024, QB), BF),
        vm((1024, HEAD), F32), vm((1024, HEAD), F32),
        vm((4, 512, COLS), BF), vm((4, 512, COLS), BF), vm((2, 512, COLS), BF), vm((2, 512, COLS), BF),
        vm((2, 256, COLS), BF), vm((2, 256, COLS), BF), vm((2, 256, COLS), F32),
        vm((512, COLS), F32), vm((3, 128, COLS), BF), vm((3, 128, COLS), BF), vm((128, COLS), F32),
        vm((128, COLS), BF), vm((128, COLS), BF),
        vm((4, 128, 1024), BF), vm((4, 128, 1024), BF), vm((4, 128, 1024), F32), vm((3, 128, 1024), BF),
        vm((16, 8, 128), F32), vm((16, 8, 128), F32),
    ]
    shapes = [(3,), (3,), (4, 3), (4,), (3,), (4,), (2, 2, 5), (2, 2, 5), (4,), (2,), (2, 2), (3,), (), (8,), (6,), (15,), (15,)]
    for shape in shapes:
        scratch += [pltpu.SemaphoreType.DMA(shape)] * 2
    whole = pl.BlockSpec(memory_space=pltpu.VMEM)
    return pl.pallas_call(
        kernel,
        out_shape=(
            jax.ShapeDtypeStruct((1, 128, MODEL_FEATURES), BF),
            jax.ShapeDtypeStruct((128, 384), F32),
            jax.ShapeDtypeStruct((128, 128), F32),
            jax.ShapeDtypeStruct((128, 128), F32),
        ),
        in_specs=[pl.BlockSpec(memory_space=pltpu.HBM)] * 11,
        out_specs=(whole,) * 4,
        scratch_shapes=scratch,
        compiler_params=pltpu.CompilerParams(
            collective_id=0, has_side_effects=True, vmem_limit_bytes=53 * 1024 * 1024 + 768 * 1024
        ),
        name="block",
    )(*args)


def solution(mesh):
    torus = Mesh(mesh.devices.reshape(4, 4, 2, 4, 2), AXES)
    in_specs = (
        P(DP, TENSOR, None),
        P(DP, None, TENSOR),
        P(DP, None, TENSOR),
        P(DP, None, TENSOR),
        P(DP, None, TENSOR),
        P(DP, TENSOR),
        P(DP, TENSOR),
        P(DP, TENSOR),
        P(DP, TENSOR),
        P(DP, TENSOR),
        P(DP, TENSOR),
    )
    out_specs = (P(DP, TENSOR, None), P(DP, TENSOR), P(DP, TENSOR), P(DP, TENSOR))
    return jax.shard_map(local, mesh=torus, in_specs=in_specs, out_specs=out_specs, check_vma=False)
```

```python
import functools
import math

import jax
import jax.numpy as jnp
from jax import lax
from jax.experimental import pallas as pl
from jax.experimental.pallas import tpu as pltpu
from jax.sharding import Mesh
from jax.sharding import PartitionSpec as P

MODEL_FEATURES = 4096
QUERY_HEADS = 24
KEY_VALUE_HEADS = 8
HEAD = 128
DP = ("dp_0", "dp_1", "dp_2")
TENSOR = ("tensor_0", "tensor_1")
AXES = DP + TENSOR
MESH = pl.DeviceIdType.MESH
BF = jnp.bfloat16
F32 = jnp.float32

COLS = 640
ALL = 4 * COLS
QB = 256


def dot(a, b, ca, cb):
    return lax.dot_general(a, b, (((ca,), (cb,)), ((), ())), preferred_element_type=F32)


def lanes(start, size):
    return pl.ds(pl.multiple_of(start, 128), size)


def kernel(
    in_ref, q_hbm, k_hbm, v_hbm, do_hbm, wq_ref, wk_ref, wv_ref, mq_hbm, mk_hbm, mv_hbm,
    gx_ref, vq_ref, vk_ref, vv_ref,
    q_ref, k_ref, v_ref, do_ref, mq_ref, mk_ref, mv_ref, l_sem, lw_sem, lx_sem,
    xq, xt, g, w, s_buf, dp_buf, p_buf, ds_buf, dk_acc, dv_acc,
    dw_cs, dw_cr, dw_xs, dw_xr, dw_vs, dw_vr, dw_h, dw_acc, dw_zs, dw_zr, dw_fin, dw_sw, dw_gr,
    dx_s, dx_r, dx_o, dx_f, sq1, sq2,
    ws_s, ws_r, wz_s, wz_r, wx_s, wx_r, wc_s, wc_r,
    xy_s, xy_r, xz_s, xz_r, go_s, go_r, gf_s, gf_r,
    dc_s, dc_r, dv_s, dv_r, dxx_s, dxx_r, dz_s, dz_r, dsw_s, dsw_r,
    ez_s, ez_r, ey_s, ey_r, s1_s, s1_r, s2_s, s2_r,
):
    x, zl, c, y, zh = (lax.axis_index(a) for a in AXES)
    scaling = 1.0 / math.sqrt(HEAD)
    other_c, other_zh = 1 - c, 1 - zh

    def at(dx=0, dl=0, dy=0):
        return (lax.rem(x + dx, 4), lax.rem(zl + dl, 4), c, lax.rem(y + dy, 4), zh)

    pair, across = zl + 1 - 2 * lax.rem(zl, 2), lax.rem(zl + 2, 4)
    blocks = (zl, across, pair, 3 - zl)
    pair_dev = (x, pair, c, y, zh)
    across_dev = (x, across, c, y, zh)
    swap_dev = (y, zl, c, x, zh)
    core_dev = (x, zl, other_c, y, zh)
    zh_dev = (x, zl, c, y, other_zh)

    def line(dz, dc):
        z = lax.rem(zh * 4 + zl + dz, 8)
        return (x, lax.rem(z, 4), lax.rem(c + dc, 2), y, z // 4)

    plane = [(dx, dy) for dx in range(4) for dy in range(4) if dx or dy]
    column = [(dz, dc) for dz in range(8) for dc in range(2) if dz or dc]

    def send(src, dst, ss, rs, dev):
        return pltpu.make_async_remote_copy(
            src_ref=src, dst_ref=dst, send_sem=ss, recv_sem=rs, device_id=dev, device_id_type=MESH
        )

    barrier = pltpu.get_barrier_semaphore()
    for dx, dy in plane:
        pl.semaphore_signal(barrier, inc=1, device_id=at(dx=dx, dy=dy), device_id_type=MESH)
    for dz, dc in column:
        pl.semaphore_signal(barrier, inc=1, device_id=line(dz, dc), device_id_type=MESH)
    loads = [
        pltpu.make_async_copy(src, dst, l_sem.at[n])
        for n, (src, dst) in enumerate(
            (
                (q_hbm, q_ref), (k_hbm, k_ref), (v_hbm, v_ref), (do_hbm, do_ref),
                (mq_hbm, mq_ref), (mk_hbm, mk_ref), (mv_hbm, mv_ref),
            )
        )
    ]
    for load in loads:
        load.start()
    pl.semaphore_wait(barrier, 30)

    w_rows = pl.ds(zl * 128, 128)
    w_parts = ((wq_ref, 0, 384), (wk_ref, 384, 128), (wv_ref, 512, 128))

    def w_swap(n):
        ref, off, size = w_parts[n]
        dst = w.at[c, w_rows, lanes(y * COLS + off, size)]
        return send(ref, dst, ws_s.at[n], ws_r.at[n], swap_dev)

    def w_here(n):
        ref, off, size = w_parts[n]
        return pltpu.make_async_copy(ref, w.at[c, w_rows, lanes(x * COLS + off, size)], lw_sem.at[n])

    def w_block(m):
        return w.at[c, pl.ds(blocks[m] * 128, 128), lanes(x * COLS, COLS)]

    def w_near(m):
        block = w_block((None, 0, 0, 1)[m])
        dev = across_dev if m == 1 else pair_dev
        return send(block, block, wz_s.at[m - 1], wz_r.at[m - 1], dev)

    def w_far(m, n):
        return send(w_block(m), w_block(m), wx_s.at[m, n], wx_r.at[m, n], at(dx=n + 1))

    def w_core(n):
        part = w.at[c, :, lanes(lax.rem(x + 4 - n, 4) * COLS, COLS)]
        return send(part, part, wc_s.at[n], wc_r.at[n], core_dev)

    @pl.when(x != y)
    def _():
        for n in range(3):
            w_swap(n).start()

    @pl.when(x == y)
    def _():
        for n in range(3):
            w_here(n).start()

    def x_rows(dy):
        return pl.ds((2 * lax.rem(y + 4 - dy, 4) + zh) * 128, 128)

    def x_y(n):
        to = lax.rem(y + n + 1, 4)
        return send(
            in_ref.at[0, :, lanes(to * 1024, 1024)], xq.at[x_rows(0)],
            xy_s.at[n], xy_r.at[n], at(dy=n + 1),
        )

    def x_z(n):
        rows = xq.at[x_rows(n)]
        return send(rows, rows, xz_s.at[n], xz_r.at[n], zh_dev)

    own_x = in_ref.at[0, :, lanes(y * 1024, 1024)]
    send(own_x, xq.at[x_rows(0)], xz_s.at[0], xz_r.at[0], zh_dev).start()
    for n in range(3):
        x_y(n).start()
    x_here = pltpu.make_async_copy(own_x, xq.at[x_rows(0)], lx_sem)
    x_here.start()
    for load in loads[:4]:
        load.wait()

    def g_own(t, p, d):
        piece = g.at[:, (other_zh, zh)[t], :, lanes(y * COLS + p * 128, 128)]
        return send(piece, piece, go_s.at[t, d, p], go_r.at[t, d, p], at(dy=1 if d == 0 else 3))

    def g_forward(t, p, d):
        of = lax.rem(y + (3 if d == 0 else 1), 4)
        half = g.at[2 * d : 2 * d + 2, (other_zh, zh)[t], :, lanes(of * COLS + p * 128, 128)]
        return send(half, half, gf_s.at[t, d, p], gf_r.at[t, d, p], at(dy=1 if d == 0 else 3))

    dk_acc[...] = jnp.zeros_like(dk_acc)
    dv_acc[...] = jnp.zeros_like(dv_acc)
    causal = lax.broadcasted_iota(jnp.int32, (QB, QB), 0) <= lax.broadcasted_iota(
        jnp.int32, (QB, QB), 1
    )

    def head(h, _):
        cols = lanes(h * HEAD, HEAD)
        for i in range(4):
            rows = pl.ds(i * QB, QB)
            qi, doi = q_ref[0, rows, cols], do_ref[0, rows, cols]
            width = (i + 1) * QB
            top = None
            for j in range(i + 1):
                js = pl.ds(j * QB, QB)
                s = dot(k_ref[0, js, :], qi, 1, 1) * scaling
                if j == i:
                    s = jnp.where(causal, s, -jnp.inf)
                s_buf[js, :] = s
                m = jnp.max(s, axis=0, keepdims=True)
                top = m if top is None else jnp.maximum(top, m)
            total = jnp.zeros((1, QB), F32)
            delta = jnp.zeros((1, QB), F32)
            for j in range(i + 1):
                js = pl.ds(j * QB, QB)
                e = jnp.exp(s_buf[js, :] - top)
                dp = dot(v_ref[0, js, :], doi, 1, 1)
                s_buf[js, :] = e
                dp_buf[js, :] = dp
                total = total + jnp.sum(e, axis=0, keepdims=True)
                delta = delta + jnp.sum(e * dp, axis=0, keepdims=True)
            inverse = 1.0 / total
            delta = delta * inverse
            for j in range(i + 1):
                js = pl.ds(j * QB, QB)
                p = s_buf[js, :] * inverse
                p_buf[js, :] = p.astype(BF)
                ds_buf[js, :] = (p * (dp_buf[js, :] - delta) * scaling).astype(BF)
            dv_acc[:width, :] += dot(p_buf[:width, :], doi, 1, 0)
            dk_acc[:width, :] += dot(ds_buf[:width, :], qi, 1, 0)
            dq = dot(ds_buf[:width, :], k_ref[0, :width, :], 0, 0).astype(BF)
            g[i, :, :, lanes(y * COLS + h * HEAD, HEAD)] = dq.reshape(2, 128, HEAD)
        @pl.when(h == 0)
        def _():
            @pl.when(x != y)
            def _():
                for n in range(3):
                    w_swap(n).wait()

            @pl.when(x == y)
            def _():
                for n in range(3):
                    w_here(n).wait()

            w_near(1).start()
            w_near(2).start()
            for n in range(3):
                w_far(0, n).start()

        g_own(0, h, 0).start()
        g_own(0, h, 1).start()
        return 0

    lax.fori_loop(0, 3, head, 0)
    for p, acc in ((3, dk_acc), (4, dv_acc)):
        g[:, :, :, lanes(y * COLS + p * 128, 128)] = acc[...].astype(BF).reshape(4, 2, 128, 128)
        g_own(0, p, 0).start()
        g_own(0, p, 1).start()

    def turn(t, _):
        rows = pl.ds(pl.multiple_of(t * 128, 128), 128)
        for b in range(8):
            block = xq[rows, b * 128 : b * 128 + 128]
            xt[b % 2, (b // 2) * 128 : (b // 2) * 128 + 128, lanes(t * 128, 128)] = block.T
        return 0

    def forward(t, p):
        for d in range(2):
            g_own(t, p, d).wait_recv()
            g_forward(t, p, d).start()

    def spread(m):
        w_near(m).wait_recv()
        if m == 1:
            w_near(3).start()
        for n in range(3):
            w_far(m, n).start()

    spread(1)
    for n in range(3):
        x_y(n).wait_recv()
    spread(2)
    for n in range(3):
        x_z(n + 1).start()
    for p in range(5):
        forward(0, p)
    for p in range(5):
        for d in range(2):
            g_own(1, p, d).start()
    spread(3)
    w_core(0).start()
    x_here.wait()
    lax.fori_loop(0, 4, lambda b, _: turn(2 * b + zh, 0), 0)
    def d_core(j):
        return send(dw_cs.at[j], dw_cr.at[j], dc_s.at[j], dc_r.at[j], core_dev)

    def d_x(d, half):
        rows = pl.ds(256 * half, 256)
        return send(
            dw_xs.at[d, rows], dw_xr.at[d, rows], dxx_s.at[d, half], dxx_r.at[d, half],
            at(dx=1 if d == 0 else 3),
        )

    def d_via(d):
        return send(dw_vs.at[d], dw_vr.at[d], dv_s.at[d], dv_r.at[d], at(dx=1 if d == 0 else 3))

    def d_z(n):
        dev = across_dev if n == 2 else pair_dev
        return send(dw_zs.at[n], dw_zr.at[n], dz_s.at[n], dz_r.at[n], dev)

    def d_swap():
        return send(dw_sw, dw_gr, dsw_s, dsw_r, swap_dev)

    def product(half, k):
        rhs = g[:, :, :, lanes(k * COLS, COLS)].reshape(1024, COLS)
        return dot(xt[half], rhs, 1, 0)

    def for_core(j):
        dw_cs[j] = product(other_c, lax.rem(y + j, 4)).astype(BF)
        d_core(j).start()

    def for_x(n):
        k = lax.rem(x + n, 4)
        j = lax.rem(k + 4 - y, 4)
        part = product(c, k)
        d_core(j).wait_recv()
        return part + dw_cr[j].astype(F32)

    def e_z(q):
        to, rows = lax.rem(y + 1 + q // 2, 4), pl.ds((q % 2) * 64, 64)
        return send(dx_s.at[to, rows], dx_r.at[to, rows], ez_s.at[q], ez_r.at[q], zh_dev)

    def e_y(q):
        rows = pl.ds((q % 2) * 64, 64)
        dst = gx_ref.at[0, rows, lanes(y * 1024, 1024)]
        return send(dx_f.at[q // 2, rows], dst, ey_s.at[q], ey_r.at[q], at(dy=q // 2 + 1))

    def back(tokens, half):
        return dot(g[:, tokens].reshape(512, ALL), w[half], 1, 1)

    for p in range(3):
        forward(1, p)
    for n in range(3):
        for m in range(4):
            w_far(m, n).wait_recv()
        w_core(n + 1).start()
    forward(1, 3)
    forward(1, 4)
    for p in range(5):
        for d in range(2):
            g_forward(0, p, d).wait_recv()
    for n in range(4):
        w_core(n).wait()
    for half in range(2):
        r = back(other_zh, half).astype(BF).reshape(4, 128, 512)
        for b in range(4):
            dx_s[:, :, b * 256 + half * 128 : b * 256 + half * 128 + 128] = r[:, :, b * 128 : b * 128 + 128]
    for q in range(4):
        e_z(q).start()
    for n in range(4):
        x_z(n).wait_recv()
    lax.fori_loop(0, 4, lambda b, _: turn(2 * b + other_zh, 0), 0)
    for j in (0, 1, 3):
        for_core(j)
    for p in range(5):
        for d in range(2):
            g_forward(1, p, d).wait_recv()
    for_core(2)
    far = for_x(2)
    for d in range(2):
        dw_vs[d] = far[256 * d : 256 * d + 256].astype(BF)
        d_via(d).start()
    for d in range(2):
        near = for_x(1 if d == 0 else 3)
        dw_xs[d, pl.ds(256 * (1 - d), 256)] = near[256 * (1 - d) : 256 * (1 - d) + 256].astype(BF)
        d_x(d, 1 - d).start()
        dw_h[d] = near[256 * d : 256 * d + 256]
    dw_acc[...] = for_x(0)
    for half in range(2):
        r = back(zh, half).reshape(4, 128, 512)
        for b in range(4):
            dx_o[:, :, b * 256 + half * 128 : b * 256 + half * 128 + 128] = r[:, :, b * 128 : b * 128 + 128]

    def finish(q):
        e_z(q).wait_recv()
        to, rows = lax.rem(y + 1 + q // 2, 4), pl.ds((q % 2) * 64, 64)
        done = (dx_o[to, rows] + dx_r[to, rows].astype(F32)).astype(BF)
        if q < 6:
            dx_f[q // 2, rows] = done
            e_y(q).start()
        else:
            gx_ref[0, rows, lanes(y * 1024, 1024)] = done

    for d in range(2):
        d_via(d).wait_recv()
        dw_xs[d, pl.ds(256 * d, 256)] = (dw_h[d] + dw_vr[d].astype(F32)).astype(BF)
        d_x(d, d).start()
    e_z(4).start()
    e_z(5).start()
    for q in range(4):
        finish(q)
    for d in range(2):
        for half in range(2):
            d_x(d, half).wait_recv()

    def summed(rows):
        r = dw_acc[rows, :]
        for d in range(2):
            r = r + dw_xr[d, rows, :].astype(F32)
        return r

    for n, to in ((1, 3), (0, 2)):
        dw_zs[n] = summed(pl.ds(blocks[to] * 128, 128)).astype(BF)
        d_z(n).start()
    rest = summed(pl.ds(across * 128, 128))
    d_z(1).wait_recv()
    dw_zs[2] = (rest + dw_zr[1].astype(F32)).astype(BF)
    d_z(2).start()
    dw_fin[...] = summed(pl.ds(zl * 128, 128))
    finish(4)
    finish(5)
    d_z(0).wait_recv()
    d_z(2).wait_recv()
    grad = dw_fin[...] + dw_zr[0].astype(F32) + dw_zr[2].astype(F32)
    dw_sw[...] = grad.astype(BF)

    @pl.when(x != y)
    def _():
        d_swap().start()

    @pl.when(x == y)
    def _():
        dw_gr[...] = dw_sw[...]

    def s_plane(n):
        return send(sq2.at[0], sq2.at[n + 1], s2_s.at[n], s2_r.at[n], at(dx=plane[n][0], dy=plane[n][1]))

    def s_column(n):
        return send(sq1.at[0], sq1.at[n + 1], s1_s.at[n], s1_r.at[n], line(*column[n]))

    squares = jnp.sum((grad * grad).reshape(16, 8, COLS), axis=0)
    sq1[0] = sum(squares[:, b * 128 : b * 128 + 128] for b in range(5))
    for n in range(15):
        s_column(n).start()
    e_z(6).start()
    for n in range(15):
        s_column(n).wait_recv()
    sq2[0] = jnp.sum(sq1[...], axis=0)
    for n in range(15):
        s_plane(n).start()
    e_z(7).start()

    for n in range(15):
        s_plane(n).wait_recv()
    squared_total = jnp.sum(jnp.sum(sq2[...], axis=0), keepdims=True)
    entries = MODEL_FEATURES * (QUERY_HEADS + 2 * KEY_VALUE_HEADS) * HEAD
    factor = 1.0 / jnp.maximum(jnp.sqrt(squared_total / entries), 1.0)

    @pl.when(x != y)
    def _():
        d_swap().wait()

    for load in loads[4:]:
        load.wait()
    vq_ref[...] = 0.9 * mq_ref[...] + factor * dw_gr[:, :384].astype(F32)
    vk_ref[...] = 0.9 * mk_ref[...] + factor * dw_gr[:, 384:512].astype(F32)
    vv_ref[...] = 0.9 * mv_ref[...] + factor * dw_gr[:, 512:].astype(F32)
    finish(6)
    finish(7)

    for n in range(3):
        x_y(n).wait_send()
        d_z(n).wait_send()
        w_near(n + 1).wait_send()
        for m in range(4):
            w_far(m, n).wait_send()
    for n in range(4):
        x_z(n).wait_send()
        d_core(n).wait_send()
    for q in range(8):
        e_z(q).wait_send()
    for q in range(6):
        e_y(q).wait()
    for d in range(2):
        d_via(d).wait_send()
        for half in range(2):
            d_x(d, half).wait_send()
    for p in range(5):
        for d in range(2):
            for t in range(2):
                g_own(t, p, d).wait_send()
                g_forward(t, p, d).wait_send()
    for n in range(15):
        s_plane(n).wait_send()
        s_column(n).wait_send()


def local(*args):
    vm = pltpu.VMEM
    scratch = [
        vm((1, 1024, 384), BF), vm((1, 1024, HEAD), BF), vm((1, 1024, HEAD), BF), vm((1, 1024, 384), BF),
        vm((128, 384), F32), vm((128, HEAD), F32), vm((128, HEAD), F32),
        pltpu.SemaphoreType.DMA((7,)), pltpu.SemaphoreType.DMA((3,)), pltpu.SemaphoreType.DMA,
        vm((1024, 1024), BF), vm((2, 512, 1024), BF), vm((4, 2, 128, ALL), BF), vm((2, 512, ALL), BF),
        vm((1024, QB), F32), vm((1024, QB), F32), vm((1024, QB), BF), vm((1024, QB), BF),
        vm((1024, HEAD), F32), vm((1024, HEAD), F32),
        vm((4, 512, COLS), BF), vm((4, 512, COLS), BF), vm((2, 512, COLS), BF), vm((2, 512, COLS), BF),
        vm((2, 256, COLS), BF), vm((2, 256, COLS), BF), vm((2, 256, COLS), F32),
        vm((512, COLS), F32), vm((3, 128, COLS), BF), vm((3, 128, COLS), BF), vm((128, COLS), F32),
        vm((128, COLS), BF), vm((128, COLS), BF),
        vm((4, 128, 1024), BF), vm((4, 128, 1024), BF), vm((4, 128, 1024), F32), vm((3, 128, 1024), BF),
        vm((16, 8, 128), F32), vm((16, 8, 128), F32),
    ]
    shapes = [(3,), (3,), (4, 3), (4,), (3,), (4,), (2, 2, 5), (2, 2, 5), (4,), (2,), (2, 2), (3,), (), (8,), (6,), (15,), (15,)]
    for shape in shapes:
        scratch += [pltpu.SemaphoreType.DMA(shape)] * 2
    whole = pl.BlockSpec(memory_space=pltpu.VMEM)
    return pl.pallas_call(
        kernel,
        out_shape=(
            jax.ShapeDtypeStruct((1, 128, MODEL_FEATURES), BF),
            jax.ShapeDtypeStruct((128, 384), F32),
            jax.ShapeDtypeStruct((128, 128), F32),
            jax.ShapeDtypeStruct((128, 128), F32),
        ),
        in_specs=[pl.BlockSpec(memory_space=pltpu.HBM)] * 11,
        out_specs=(whole,) * 4,
        scratch_shapes=scratch,
        compiler_params=pltpu.CompilerParams(
            collective_id=0, has_side_effects=True, vmem_limit_bytes=53 * 1024 * 1024 + 768 * 1024
        ),
        name="block",
    )(*args)


def solution(mesh):
    torus = Mesh(mesh.devices.reshape(4, 4, 2, 4, 2), AXES)
    in_specs = (
        P(DP, TENSOR, None),
        P(DP, None, TENSOR),
        P(DP, None, TENSOR),
        P(DP, None, TENSOR),
        P(DP, None, TENSOR),
        P(DP, TENSOR),
        P(DP, TENSOR),
        P(DP, TENSOR),
        P(DP, TENSOR),
        P(DP, TENSOR),
        P(DP, TENSOR),
    )
    out_specs = (P(DP, TENSOR, None), P(DP, TENSOR), P(DP, TENSOR), P(DP, TENSOR))
    return jax.shard_map(local, mesh=torus, in_specs=in_specs, out_specs=out_specs, check_vma=False)
```
